1024 devices in a mesh: section: 16 (over y, core), dp: 4 (over z_lo), tensor: 16 (over x, z_hi).
Axes of the slice: x: 4, y: 8, z: 16 (z_hi: 4, z_lo: 4; z = z_hi * 4 + z_lo), core: 2. Of those that a mesh axis runs over, the one named last changes fastest.
Arguments:
- shadow_weight_copy: bfloat16 [16, 4096, 4096], P('section', None, 'tensor'), may hold values from -6 to 6
- newest_weight_version: bfloat16 [16, 4096, 4096], P('section', 'dp', 'tensor'), may hold values from -6 to 6
- momentum: bfloat16 [16, 4096, 4096], P('section', 'dp', 'tensor'), may hold values from -3 to 3
- pending_section_input: bfloat16 [4, 16, 64, 4096], P('dp', 'section', None, 'tensor'), may hold values from -16 to 16
- incoming_micro_input: bfloat16 [4, 3, 64, 4096], P('dp', None, None, 'tensor'), may hold values from -16 to 16
- pending_output_gradient: bfloat16 [4, 16, 64, 4096], P('dp', 'section', None, 'tensor'), may hold values from -16 to 16
- loss_gradient_rows: bfloat16 [4, 3, 64, 4096], P('dp', None, None, 'tensor'), may hold values from -16 to 16
- stashed: bfloat16 [4, 16, 4, 64, 4096], P('dp', 'section', None, None, 'tensor'), may hold values from -16 to 16
Outputs:
- forward_out: bfloat16 [4, 16, 4, 64, 4096], P('dp', 'section', None, None, 'tensor')
- backward_out: bfloat16 [4, 16, 4, 64, 4096], P('dp', 'section', None, None, 'tensor')
- w_next: bfloat16 [16, 4096, 4096], P('section', 'dp', 'tensor')
- m_next: bfloat16 [16, 4096, 4096], P('section', 'dp', 'tensor')
The draws below stay inside these ranges and needn't reach their ends.
All inputs are finite; a program needn't handle non-finite values.
Results may differ from the reference program's by a relative error of at most 0.025.
Values may be sent and summed in bfloat16 or wider, within the bound.
A program may use at most 64 MiB of HBM per device.

```python
import math
import jax
import jax.numpy as jnp
from jax import lax

D = 4096
ROWS = 64
TICKS = 4
SECTIONS = 16
REPLICAS = 4
N_TENSOR = 16


def feature_field(key, dimensions):
    extent = dimensions[-1]
    random_part = jax.random.normal(jax.random.fold_in(key, 1), dimensions, jnp.float32)
    growth = jnp.exp(jnp.log(3.0) * jnp.arange(extent, dtype=jnp.float32) / (extent - 1))
    result_field = random_part * growth / jnp.sqrt(jnp.mean(growth * growth))
    return jnp.clip(result_field, -16.0, 16.0).astype(jnp.bfloat16)


def draw_pending_section_input(key, part):
    return feature_field(jax.random.fold_in(key, 101), (REPLICAS, SECTIONS, ROWS, D))


def draw_incoming_micro_input(key, part):
    return feature_field(jax.random.fold_in(key, 102), (REPLICAS, TICKS - 1, ROWS, D))


def draw_pending_output_gradient(key, part):
    return feature_field(jax.random.fold_in(key, 103), (REPLICAS, SECTIONS, ROWS, D))


def draw_loss_gradient_rows(key, part):
    return feature_field(jax.random.fold_in(key, 104), (REPLICAS, TICKS - 1, ROWS, D))


def draw_stashed(key, part):
    return feature_field(jax.random.fold_in(key, 105), (REPLICAS, SECTIONS, TICKS, ROWS, D))


def block_scale(rng, dims, cuts, least, largest):
    gain, own = 1.0, jax.random.fold_in(rng, 6)
    for position, shards_of in cuts:
        steps = jnp.exp(jax.random.uniform(jax.random.fold_in(own, position), (shards_of,), jnp.float32, least / len(cuts), largest / len(cuts)))
        gain = gain * jnp.repeat(steps, dims[position] // shards_of).reshape([-1 if axis == position else 1 for axis in range(len(dims))])
    return gain


def scatter_about(own_key, shape, spread, bound, split=(), kind=jnp.bfloat16):
    values = spread * jax.random.normal(own_key, shape, jnp.float32)
    if split:
        values = values * block_scale(own_key, shape, split, -0.22, 0.18)
    return jnp.clip(values, -bound, bound).astype(kind)


def setup_inputs(seed: int = 0) -> dict:
    streams_of = jax.random.split(jax.random.key(seed), 9)
    shadow_weight_copy = scatter_about(streams_of[0], (SECTIONS, D, D), 1.0, 6.0, ((0, 16), (2, 16)))
    newest_weight_version = scatter_about(streams_of[1], (SECTIONS, D, D), 1.0, 6.0, ((0, 16), (1, 4), (2, 16)))
    momentum = scatter_about(streams_of[2], (SECTIONS, D, D), 0.5, 3.0, ((0, 16), (1, 4), (2, 16)))
    pending_section_input = draw_pending_section_input(jax.random.fold_in(streams_of[8], 71), 0)
    incoming_micro_input = draw_incoming_micro_input(jax.random.fold_in(streams_of[8], 71), 0)
    pending_output_gradient = draw_pending_output_gradient(jax.random.fold_in(streams_of[8], 71), 0)
    loss_gradient_rows = draw_loss_gradient_rows(jax.random.fold_in(streams_of[8], 71), 0)
    stashed = draw_stashed(jax.random.fold_in(streams_of[8], 71), 0)
    return {"shadow_weight_copy": shadow_weight_copy, "newest_weight_version": newest_weight_version, "momentum": momentum, "pending_section_input": pending_section_input, "incoming_micro_input": incoming_micro_input, "pending_output_gradient": pending_output_gradient, "loss_gradient_rows": loss_gradient_rows, "stashed": stashed}


EPSILON = 1e-06
MOMENTUM_RATE = 0.9
LEARNING_RATE = 0.05

def normalized(values):
    factor = lax.rsqrt(lax.optimization_barrier(jnp.mean(values * values, axis=-1, keepdims=True)) + EPSILON)
    return (values * factor, factor)

def rounded(values):
    return lax.optimization_barrier(values.astype(jnp.bfloat16)).astype(jnp.float32)

def section_tick(operands):
    current_input, kept_in, grad_in, weight = operands
    extent = weight.shape[0]
    root_width = math.sqrt(extent)
    weight_wide = weight.astype(jnp.float32)
    x_wide = current_input.astype(jnp.float32)
    x_hat, unused = normalized(x_wide)
    branch = jnp.einsum('prd,de->pre', rounded(x_hat), weight_wide) / root_width
    section_out = (x_wide + branch).astype(jnp.bfloat16)
    kept_hat, kept_factor = normalized(kept_in.astype(jnp.float32))
    grad_wide = grad_in.astype(jnp.float32)
    replicas = grad_in.shape[0]
    row_count = grad_in.shape[1]
    shard_cols = extent // N_TENSOR
    grad_pieces = grad_wide.reshape(replicas, row_count, N_TENSOR, shard_cols)
    weight_pieces = weight_wide.reshape(extent, N_TENSOR, shard_cols)
    partial_value = jnp.einsum('prje,dje->pjrd', grad_pieces, weight_pieces) / root_width
    branch_grad = lax.optimization_barrier(jnp.sum(rounded(partial_value), axis=1))
    inner_dot = lax.optimization_barrier(jnp.mean(branch_grad * kept_hat, axis=-1, keepdims=True))
    input_grad = (grad_wide + (branch_grad - kept_hat * inner_dot) * kept_factor).astype(jnp.bfloat16)
    return (section_out, input_grad, kept_hat.astype(jnp.bfloat16))

def section_update(operands):
    kept_rows, grad_rows, latest, moment = operands
    extent = latest.shape[0]
    replica_terms = jnp.einsum('pkrd,pkre->pde', kept_rows.astype(jnp.float32), grad_rows.astype(jnp.float32)) / math.sqrt(extent)
    summed = lax.optimization_barrier(jnp.sum(rounded(replica_terms), axis=0))
    velocity = MOMENTUM_RATE * moment.astype(jnp.float32) + summed
    new_weight = (latest.astype(jnp.float32) - LEARNING_RATE * velocity).astype(jnp.bfloat16)
    return (new_weight, velocity.astype(jnp.bfloat16))

def reference(shadow_weight_copy, newest_weight_version, momentum, pending_section_input, incoming_micro_input, pending_output_gradient, loss_gradient_rows, stashed):
    tick_count = stashed.shape[2]
    current_input = pending_section_input
    current_gradient = pending_output_gradient
    forward_list = []
    backward_list = []
    kept_list = []
    grad_list = []
    for tick_index in range(tick_count):
        if tick_index > 0:
            current_input = jnp.concatenate([incoming_micro_input[:, tick_index - 1][:, None], forward_list[-1][:, :-1]], axis=1)
            current_gradient = jnp.concatenate([backward_list[-1][:, 1:], loss_gradient_rows[:, tick_index - 1][:, None]], axis=1)
        operands = (jnp.moveaxis(current_input, 1, 0), jnp.moveaxis(stashed[:, :, tick_index], 1, 0), jnp.moveaxis(current_gradient, 1, 0), shadow_weight_copy)
        section_out, input_grad, kept_norm = lax.map(section_tick, operands)
        forward_list.append(jnp.moveaxis(section_out, 0, 1))
        backward_list.append(jnp.moveaxis(input_grad, 0, 1))
        kept_list.append(jnp.moveaxis(kept_norm, 0, 1))
        grad_list.append(current_gradient)
    forward_out = jnp.stack(forward_list, axis=2)
    backward_out = jnp.stack(backward_list, axis=2)
    kept_all = jnp.stack(kept_list, axis=2)
    grad_all = jnp.stack(grad_list, axis=2)
    w_next, m_next = lax.map(section_update, (jnp.moveaxis(kept_all, 1, 0), jnp.moveaxis(grad_all, 1, 0), newest_weight_version, momentum))
    return (forward_out, backward_out, w_next, m_next)
```

```python
import functools

import jax
import jax.numpy as jnp
from jax import lax
from jax.experimental import pallas as pl
from jax.experimental.pallas import tpu as pltpu
from jax.sharding import PartitionSpec as P

EPSILON = 1e-06
MOMENTUM_RATE = 0.9
LEARNING_RATE = 0.05
MESH = pl.DeviceIdType.MESH
F32 = jnp.float32
BF16 = jnp.bfloat16

SIDE = 4
NEAR_LAST = (2, 1, 3, 0)
NEAR_FIRST = (0, 1, 3, 2)


def local_wait(ref, sem):
    pltpu.make_async_copy(ref, ref, sem).wait()


def kernel(
    w_in, new_in, mom_in, x_in, inc_in, g_in, loss_in, kept_in,
    f_out, b_out, w_out, m_out,
    w, x, kept, part, part_in, half, half_in, grad, f_own, b_own, f_send, b_send,
    inc, loss, scaled, p1, p1_in, p2, p2_in, kw, keep0, dw, dw_in, new, mom, w_new, m_new,
    load, fz_r, fz_s, fx_r, fx_s, kz_r, kz_s, kx_r, kx_s, rx_r, rx_s, rz_r, rz_s,
    p1_r, p1_s, p2_r, p2_s, g_r, g_s, dp_r, dp_s, out_sem,
):
    blocks, depth, own_cols = w.shape
    ticks, rows = x.shape[0], x.shape[2]
    extent = blocks * depth
    inv_root = 1.0 / float(extent) ** 0.5
    s, r, j = lax.axis_index("section"), lax.axis_index("dp"), lax.axis_index("tensor")
    sections, replicas = lax.axis_size("section"), lax.axis_size("dp")
    col, rank = lax.div(j, SIDE), lax.rem(j, SIDE)
    up, down = lax.rem(s + 1, sections), lax.rem(s + sections - 1, sections)
    is_first, is_last = s == 0, s == sections - 1

    def xs(e):
        return lax.rem(col + e + SIDE, SIDE)

    def zs(d):
        return lax.rem(rank + d + SIDE, SIDE)

    def remote(src, dst, send, recv, device):
        pltpu.make_async_remote_copy(
            src_ref=src, dst_ref=dst, send_sem=send, recv_sem=recv,
            device_id=device, device_id_type=MESH,
        ).start()

    barrier = pltpu.get_barrier_semaphore()
    peers = [(s, r, xs(e) * SIDE + rank) for e in range(1, SIDE)]
    peers += [(s, r, col * SIDE + zs(d)) for d in range(1, SIDE)]
    peers += [(q, r, col * SIDE + zs(d)) for q in (up, down) for d in range(SIDE)]
    peers += [(s, lax.rem(r + f, replicas), j) for f in range(1, replicas)]
    for peer in peers:
        pl.semaphore_signal(barrier, inc=1, device_id=peer, device_id_type=MESH)

    loads = [
        pltpu.make_async_copy(src, dst, load.at[i])
        for i, (src, dst) in enumerate([
            (x_in, x.at[0, j]), (g_in, grad.at[0]), (kept_in, kept.at[j]), (w_in, w),
            (inc_in, inc), (loss_in, loss), (new_in, new), (mom_in, mom),
        ])
    ]
    for copy in loads:
        copy.start()
    for copy in loads[:3]:
        copy.wait()
    pl.semaphore_wait(barrier, len(peers))

    for d in NEAR_LAST[:3]:
        remote(x.at[0, j], x.at[0, j], fz_s.at[0], fz_r.at[0, d], (s, r, col * SIDE + zs(d)))

    def kept_to_z(t):
        mine = kept.at[j, pl.ds(pl.multiple_of(t * rows, rows), rows), :]
        for d in NEAR_LAST[:3]:
            remote(mine, mine, kz_s.at[t], kz_r.at[t], (s, r, col * SIDE + zs(d)))

    def kept_to_x(t):
        span = pl.ds(pl.multiple_of(t * rows, rows), rows)
        local_wait(kept.at[pl.ds(0, SIDE - 1), span, :], kz_r.at[t])
        group = kept.at[pl.ds(col * SIDE, SIDE), span, :]
        for e in NEAR_LAST[:3]:
            remote(group, group, kx_s.at[t], kx_r.at[t], (s, r, xs(e) * SIDE + rank))

    loads[3].wait()
    loads[4].wait()
    loads[5].wait()

    row_id = lax.broadcasted_iota(jnp.int32, (rows, 128), 0)
    lane_id = lax.broadcasted_iota(jnp.int32, (rows, 128), 1)
    diagonal = row_id == lane_id

    def tick(t, carry):
        @pl.when(t > 0)
        def _():
            local_wait(grad.at[0], g_r.at[t])

        g = grad[t]
        for e in NEAR_LAST:
            for d in NEAR_LAST:
                k = xs(e) * SIDE + zs(d)
                term = lax.dot_general(
                    g, w[k], (((1,), (1,)), ((), ())), preferred_element_type=F32
                )
                part[t, k] = (term * inv_root).astype(BF16)
                if e:
                    remote(
                        part.at[t, k], part_in.at[t, d, e - 1], rx_s.at[t], rx_r.at[t, d],
                        (s, r, xs(e) * SIDE + rank),
                    )

        def pass_on(d):
            k = col * SIDE + zs(-d)
            for e in NEAR_LAST[:3]:
                remote(
                    x.at[t, k], x.at[t, k], fx_s.at[t], fx_r.at[t, d],
                    (s, r, xs(e) * SIDE + rank),
                )

        @pl.when(t > 0)
        def _():
            local_wait(x.at[t, 0], fz_r.at[t, 0])

        pass_on(0)

        @pl.when(t == 0)
        def _():
            kept_to_z(t)

        for d in (1, 3):
            local_wait(x.at[t, 0], fz_r.at[t, d])
            pass_on(d)

        def over_x(d):
            local_wait(part_in.at[t, d], rx_r.at[t, d])
            total = part[t, col * SIDE + zs(d)].astype(F32)
            for e in range(SIDE - 1):
                total += part_in[t, d, e].astype(F32)
            return total

        for d in (2, 1, 3):
            half[t, d - 1] = over_x(d).astype(BF16)
            remote(
                half.at[t, d - 1], half_in.at[t, d - 1], rz_s.at[t], rz_r.at[t],
                (s, r, col * SIDE + zs(d)),
            )
        keep0[...] = over_x(0)

        local_wait(x.at[t, 0], fz_r.at[t, 2])
        pass_on(2)

        @pl.when(t == 0)
        def _():
            kept_to_x(t)

        @pl.when(t < ticks - 1)
        def _():
            kept_to_z(t + 1)

        span = pl.ds(pl.multiple_of(t * rows, rows), rows)
        local_wait(kept.at[pl.ds(0, SIDE * (SIDE - 1)), span, :], kx_r.at[t])
        kept_product = jnp.zeros((rows, own_cols), F32)
        squares = jnp.zeros((rows, own_cols), F32)
        for k in range(blocks):
            block = kept[k, span, :]
            kept_product += jnp.dot(block, w[k], preferred_element_type=F32)
            wide = block.astype(F32)
            squares += wide * wide
        kept_scale = lax.rsqrt(jnp.sum(squares, axis=-1, keepdims=True) / extent + EPSILON)
        g_wide = grad[t].astype(F32)
        scaled[span, :] = (g_wide * kept_scale).astype(BF16)
        dots = jnp.sum(g_wide * kept_product, axis=-1, keepdims=True) * kept_scale * inv_root
        p1[t] = jnp.sum(jnp.where(diagonal, dots, 0.0), axis=0, keepdims=True)
        for e in NEAR_LAST[:3]:
            remote(
                p1.at[t], p1_in.at[t, e - 1], p1_s.at[t], p1_r.at[t],
                (s, r, xs(e) * SIDE + rank),
            )

        @pl.when(t == ticks - 1)
        def _():
            right = scaled[...]
            for f in (3, 2, 1, 0):
                owner = lax.rem(r + f, replicas)
                for c in range(SIDE):
                    k = owner * SIDE + c
                    term = lax.dot_general(
                        kept[k], right, (((0,), (0,)), ((), ())), preferred_element_type=F32
                    )
                    dw[k] = (term * inv_root).astype(BF16)
                if f:
                    remote(
                        dw.at[pl.ds(owner * SIDE, SIDE)], dw_in.at[f - 1], dp_s, dp_r.at[f - 1],
                        (s, owner, j),
                    )

        total = jnp.zeros((rows, own_cols), F32)
        squares = jnp.zeros((rows, own_cols), F32)
        for d in NEAR_FIRST:
            local_wait(x.at[t, pl.ds(0, SIDE - 1)], fx_r.at[t, d])
            for e in range(SIDE):
                k = xs(-e) * SIDE + zs(-d)
                block = x[t, k]
                total += jnp.dot(block, w[k], preferred_element_type=F32)
                wide = block.astype(F32)
                squares += wide * wide
        scale = lax.rsqrt(jnp.sum(squares, axis=-1, keepdims=True) / extent + EPSILON)
        result = (x[t, j].astype(F32) + total * scale * inv_root).astype(BF16)
        f_own[t] = result

        @pl.when(t < ticks - 1)
        def _():
            f_send[t] = jnp.where(is_last, inc[jnp.minimum(t, ticks - 2)], result)
            for d in NEAR_LAST:
                remote(
                    f_send.at[t], x.at[t + 1, j], fz_s.at[t + 1], fz_r.at[t + 1, d],
                    (up, r, col * SIDE + zs(d)),
                )

        local_wait(p1_in.at[t], p1_r.at[t])
        p2[t] = p1[t] + p1_in[t, 0] + p1_in[t, 1] + p1_in[t, 2]
        for d in NEAR_LAST[:3]:
            remote(
                p2.at[t], p2_in.at[t, d - 1], p2_s.at[t], p2_r.at[t],
                (s, r, col * SIDE + zs(d)),
            )

        @pl.when(t < ticks - 1)
        def _():
            kept_to_x(t + 1)

        local_wait(half_in.at[t], rz_r.at[t])
        branch = keep0[...]
        for d in range(SIDE - 1):
            branch += half_in[t, d].astype(F32)
        local_wait(p2_in.at[t], p2_r.at[t])
        line = p2[t] + p2_in[t, 0] + p2_in[t, 1] + p2_in[t, 2]
        inner = jnp.sum(jnp.where(diagonal, line, 0.0), axis=-1, keepdims=True) / extent
        hat = kept[j, span, :].astype(F32) * kept_scale
        back = (grad[t].astype(F32) + (branch - hat * inner) * kept_scale).astype(BF16)
        b_own[t] = back

        @pl.when(t < ticks - 1)
        def _():
            b_send[t] = jnp.where(is_first, loss[jnp.minimum(t, ticks - 2)], back)
            remote(b_send.at[t], grad.at[t + 1], g_s.at[t + 1], g_r.at[t + 1], (down, r, j))

        return carry

    lax.fori_loop(0, ticks, tick, 0)

    outs = [
        pltpu.make_async_copy(f_own, f_out, out_sem.at[0]),
        pltpu.make_async_copy(b_own, b_out, out_sem.at[1]),
    ]
    for copy in outs:
        copy.start()
    loads[6].wait()
    loads[7].wait()
    for f in range(replicas - 1):
        local_wait(dw_in.at[f], dp_r.at[f])
    for c in range(SIDE):
        summed = dw[r * SIDE + c].astype(F32)
        for f in range(replicas - 1):
            summed += dw_in[f, c].astype(F32)
        velocity = MOMENTUM_RATE * mom[c].astype(F32) + summed
        w_new[c] = (new[c].astype(F32) - LEARNING_RATE * velocity).astype(BF16)
        m_new[c] = velocity.astype(BF16)
    more = [
        pltpu.make_async_copy(w_new, w_out, out_sem.at[2]),
        pltpu.make_async_copy(m_new, m_out, out_sem.at[3]),
    ]
    for copy in more:
        copy.start()

    for t in range(ticks):
        local_wait(x.at[0, pl.ds(0, SIDE if t else SIDE - 1)], fz_s.at[t])
        local_wait(x.at[0, pl.ds(0, SIDE * (SIDE - 1))], fx_s.at[t])
        local_wait(x.at[0, pl.ds(0, SIDE - 1)], kz_s.at[t])
        local_wait(x.at[0, pl.ds(0, SIDE * (SIDE - 1))], kx_s.at[t])
        local_wait(x.at[0, pl.ds(0, SIDE * (SIDE - 1))], rx_s.at[t])
        local_wait(x.at[0, pl.ds(0, SIDE - 1)], rz_s.at[t])
        local_wait(p1_in.at[0], p1_s.at[t])
        local_wait(p2_in.at[0], p2_s.at[t])
        if t:
            local_wait(grad.at[0], g_s.at[t])
    local_wait(dw_in, dp_s)
    for copy in outs + more:
        copy.wait()


def body(
    shadow_weight_copy, newest_weight_version, momentum, pending_section_input,
    incoming_micro_input, pending_output_gradient, loss_gradient_rows, stashed,
):
    extent, cols = shadow_weight_copy.shape[1:]
    ticks, rows = stashed.shape[2:4]
    part_rows = newest_weight_version.shape[1]
    replicas = extent // part_rows
    blocks = extent // cols
    chunk = part_rows // SIDE

    vmem, dma = pltpu.VMEM, pltpu.SemaphoreType.DMA
    block = (rows, cols)
    scratch = [
        vmem((blocks, cols, cols), BF16),
        vmem((ticks, blocks, *block), BF16),
        vmem((blocks, ticks * rows, cols), BF16),
        vmem((ticks, blocks, *block), BF16),
        vmem((ticks, SIDE, SIDE - 1, *block), BF16),
        vmem((ticks, SIDE - 1, *block), BF16),
        vmem((ticks, SIDE - 1, *block), BF16),
        vmem((ticks, *block), BF16),
        vmem((ticks, *block), BF16),
        vmem((ticks, *block), BF16),
        vmem((ticks - 1, *block), BF16),
        vmem((ticks - 1, *block), BF16),
        vmem((ticks - 1, *block), BF16),
        vmem((ticks - 1, *block), BF16),
        vmem((ticks * rows, cols), BF16),
        vmem((ticks, 1, 128), F32),
        vmem((ticks, SIDE - 1, 1, 128), F32),
        vmem((ticks, 1, 128), F32),
        vmem((ticks, SIDE - 1, 1, 128), F32),
        vmem(block, F32),
        vmem(block, F32),
        vmem((blocks, cols, cols), BF16),
        vmem((replicas - 1, SIDE, chunk, cols), BF16),
        vmem((SIDE, chunk, cols), BF16),
        vmem((SIDE, chunk, cols), BF16),
        vmem((SIDE, chunk, cols), BF16),
        vmem((SIDE, chunk, cols), BF16),
        dma((8,)),
        dma((ticks, SIDE)), dma((ticks,)),
        dma((ticks, SIDE)), dma((ticks,)),
        dma((ticks,)), dma((ticks,)),
        dma((ticks,)), dma((ticks,)),
        dma((ticks, SIDE)), dma((ticks,)),
        dma((ticks,)), dma((ticks,)),
        dma((ticks,)), dma((ticks,)),
        dma((ticks,)), dma((ticks,)),
        dma((ticks,)), dma((ticks,)),
        dma((replicas - 1,)), dma,
        dma((4,)),
    ]
    any_space = pl.BlockSpec(memory_space=pl.ANY)
    shape = jax.ShapeDtypeStruct
    f_out, b_out, w_out, m_out = pl.pallas_call(
        kernel,
        name="window",
        out_shape=(
            shape((ticks, *block), BF16),
            shape((ticks, *block), BF16),
            shape((SIDE, chunk, cols), BF16),
            shape((SIDE, chunk, cols), BF16),
        ),
        in_specs=[any_space] * 8,
        out_specs=(any_space,) * 4,
        scratch_shapes=scratch,
        compiler_params=pltpu.CompilerParams(
            collective_id=0, has_side_effects=True, vmem_limit_bytes=60 * 1024 * 1024
        ),
    )(
        shadow_weight_copy.reshape(blocks, cols, cols),
        newest_weight_version.reshape(SIDE, chunk, cols),
        momentum.reshape(SIDE, chunk, cols),
        pending_section_input.reshape(block),
        incoming_micro_input.reshape(ticks - 1, *block),
        pending_output_gradient.reshape(block),
        loss_gradient_rows.reshape(ticks - 1, *block),
        stashed.reshape(ticks * rows, cols),
    )
    return (
        f_out[None, None],
        b_out[None, None],
        w_out.reshape(1, part_rows, cols),
        m_out.reshape(1, part_rows, cols),
    )


def solution(mesh):
    return jax.shard_map(
        body,
        mesh=mesh,
        in_specs=(
            P("section", None, "tensor"),
            P("section", "dp", "tensor"),
            P("section", "dp", "tensor"),
            P("dp", "section", None, "tensor"),
            P("dp", None, None, "tensor"),
            P("dp", "section", None, "tensor"),
            P("dp", None, None, "tensor"),
            P("dp", "section", None, None, "tensor"),
        ),
        out_specs=(
            P("dp", "section", None, None, "tensor"),
            P("dp", "section", None, None, "tensor"),
            P("section", "dp", "tensor"),
            P("section", "dp", "tensor"),
        ),
        check_vma=False,
    )
```

```python
import functools

import jax
import jax.numpy as jnp
from jax import lax
from jax.experimental import pallas as pl
from jax.experimental.pallas import tpu as pltpu
from jax.sharding import PartitionSpec as P

EPSILON = 1e-06
MOMENTUM_RATE = 0.9
LEARNING_RATE = 0.05
MESH = pl.DeviceIdType.MESH
F32 = jnp.float32
BF16 = jnp.bfloat16

SIDE = 4
NEAR_LAST = (2, 1, 3, 0)
NEAR_FIRST = (0, 1, 3, 2)


def local_wait(ref, sem):
    pltpu.make_async_copy(ref, ref, sem).wait()


def kernel(
    w_in, new_in, mom_in, x_in, inc_in, g_in, loss_in, kept_in,
    f_out, b_out, w_out, m_out,
    w, x, kept, part, part_in, half, half_in, grad, f_own, b_own, f_send, b_send,
    inc, loss, scaled, p1, p1_in, p2, p2_in, kw, ks, keep0, dw, dw_in, new, mom, w_new, m_new,
    load, fz_r, fz_s, fx_r, fx_s, kz_r, kz_s, kx_r, kx_s, rx_r, rx_s, rz_r, rz_s,
    p1_r, p1_s, p2_r, p2_s, g_r, g_s, dp_r, dp_s, out_sem,
):
    blocks, depth, own_cols = w.shape
    ticks, rows = x.shape[0], x.shape[2]
    extent = blocks * depth
    inv_root = 1.0 / float(extent) ** 0.5
    s, r, j = lax.axis_index("section"), lax.axis_index("dp"), lax.axis_index("tensor")
    sections, replicas = lax.axis_size("section"), lax.axis_size("dp")
    col, rank = lax.div(j, SIDE), lax.rem(j, SIDE)
    up, down = lax.rem(s + 1, sections), lax.rem(s + sections - 1, sections)
    is_first, is_last = s == 0, s == sections - 1

    def xs(e):
        return lax.rem(col + e + SIDE, SIDE)

    def zs(d):
        return lax.rem(rank + d + SIDE, SIDE)

    def remote(src, dst, send, recv, device):
        pltpu.make_async_remote_copy(
            src_ref=src, dst_ref=dst, send_sem=send, recv_sem=recv,
            device_id=device, device_id_type=MESH,
        ).start()

    barrier = pltpu.get_barrier_semaphore()
    peers = [(s, r, xs(e) * SIDE + rank) for e in range(1, SIDE)]
    peers += [(s, r, col * SIDE + zs(d)) for d in range(1, SIDE)]
    peers += [(q, r, col * SIDE + zs(d)) for q in (up, down) for d in range(SIDE)]
    peers += [(s, lax.rem(r + f, replicas), j) for f in range(1, replicas)]
    for peer in peers:
        pl.semaphore_signal(barrier, inc=1, device_id=peer, device_id_type=MESH)

    loads = [
        pltpu.make_async_copy(src, dst, load.at[i])
        for i, (src, dst) in enumerate([
            (x_in, x.at[0, j]), (g_in, grad.at[0]), (kept_in, kept.at[j]), (w_in, w),
            (inc_in, inc), (loss_in, loss), (new_in, new), (mom_in, mom),
        ])
    ]
    for copy in loads:
        copy.start()
    for copy in loads[:3]:
        copy.wait()
    pl.semaphore_wait(barrier, len(peers))

    for d in NEAR_LAST[:3]:
        remote(x.at[0, j], x.at[0, j], fz_s.at[0], fz_r.at[0, d], (s, r, col * SIDE + zs(d)))

    def kept_to_z(t):
        mine = kept.at[j, pl.ds(pl.multiple_of(t * rows, rows), rows), :]
        for d in NEAR_LAST[:3]:
            remote(mine, mine, kz_s.at[t], kz_r.at[t], (s, r, col * SIDE + zs(d)))

    def kept_to_x(t):
        span = pl.ds(pl.multiple_of(t * rows, rows), rows)
        local_wait(kept.at[pl.ds(0, SIDE - 1), span, :], kz_r.at[t])
        group = kept.at[pl.ds(col * SIDE, SIDE), span, :]
        for e in NEAR_LAST[:3]:
            remote(group, group, kx_s.at[t], kx_r.at[t], (s, r, xs(e) * SIDE + rank))

    loads[3].wait()
    loads[4].wait()
    loads[5].wait()

    row_id = lax.broadcasted_iota(jnp.int32, (rows, 128), 0)
    lane_id = lax.broadcasted_iota(jnp.int32, (rows, 128), 1)
    diagonal = row_id == lane_id

    def kept_products(t):
        span = pl.ds(pl.multiple_of(t * rows, rows), rows)
        local_wait(kept.at[pl.ds(0, SIDE * (SIDE - 1)), span, :], kx_r.at[t])
        product = jnp.zeros((rows, own_cols), F32)
        squares = jnp.zeros((rows, own_cols), F32)
        for k in range(blocks):
            block = kept[k, span, :]
            product += jnp.dot(block, w[k], preferred_element_type=F32)
            wide = block.astype(F32)
            squares += wide * wide
        found = lax.rsqrt(jnp.sum(squares, axis=-1, keepdims=True) / extent + EPSILON)
        kw[...] = product * (found * inv_root)
        ks[...] = jnp.broadcast_to(found, (rows, 128))

    def row_products(t):
        span = pl.ds(pl.multiple_of(t * rows, rows), rows)
        g_wide = grad[t].astype(F32)
        scaled[span, :] = (g_wide * ks[:, :1]).astype(BF16)
        dots = jnp.sum(g_wide * kw[...], axis=-1, keepdims=True)
        p1[t] = jnp.sum(jnp.where(diagonal, dots, 0.0), axis=0, keepdims=True)
        for e in NEAR_LAST[:3]:
            remote(
                p1.at[t], p1_in.at[t, e - 1], p1_s.at[t], p1_r.at[t],
                (s, r, xs(e) * SIDE + rank),
            )

    def tick(t, carry):
        span = pl.ds(pl.multiple_of(t * rows, rows), rows)

        @pl.when(t > 0)
        def _():
            kept_products(t)
            local_wait(grad.at[0], g_r.at[t])
            row_products(t)

        @pl.when(t == ticks - 1)
        def _():
            right = scaled[...]
            for f in (2, 3, 1, 0):
                owner = lax.rem(r + f, replicas)
                for c in range(SIDE):
                    k = owner * SIDE + c
                    term = lax.dot_general(
                        kept[k], right, (((0,), (0,)), ((), ())), preferred_element_type=F32
                    )
                    dw[k] = (term * inv_root).astype(BF16)
                if f:
                    remote(
                        dw.at[pl.ds(owner * SIDE, SIDE)], dw_in.at[f - 1], dp_s, dp_r.at[f - 1],
                        (s, owner, j),
                    )

        g = grad[t]
        for d in NEAR_LAST:
            for e in NEAR_LAST:
                k = xs(e) * SIDE + zs(d)
                term = lax.dot_general(
                    g, w[k], (((1,), (1,)), ((), ())), preferred_element_type=F32
                )
                part[t, k] = (term * inv_root).astype(BF16)
                if e:
                    remote(
                        part.at[t, k], part_in.at[t, d, e - 1], rx_s.at[t], rx_r.at[t, d],
                        (s, r, xs(e) * SIDE + rank),
                    )

        def pass_on(d):
            k = col * SIDE + zs(-d)
            for e in NEAR_LAST[:3]:
                remote(
                    x.at[t, k], x.at[t, k], fx_s.at[t], fx_r.at[t, d],
                    (s, r, xs(e) * SIDE + rank),
                )

        @pl.when(t > 0)
        def _():
            local_wait(x.at[t, 0], fz_r.at[t, 0])

        pass_on(0)

        @pl.when(t == 0)
        def _():
            kept_to_z(t)

        def over_x(d):
            local_wait(part_in.at[t, d], rx_r.at[t, d])
            total = part[t, col * SIDE + zs(d)].astype(F32)
            for e in range(SIDE - 1):
                total += part_in[t, d, e].astype(F32)
            return total

        for d in (2, 1, 3):
            half[t, d - 1] = over_x(d).astype(BF16)
            remote(
                half.at[t, d - 1], half_in.at[t, d - 1], rz_s.at[t], rz_r.at[t],
                (s, r, col * SIDE + zs(d)),
            )
            if d != 2:
                local_wait(x.at[t, 0], fz_r.at[t, d])
                pass_on(d)
        keep0[...] = over_x(0)

        local_wait(x.at[t, 0], fz_r.at[t, 2])
        pass_on(2)

        @pl.when(t == 0)
        def _():
            kept_to_x(t)
            kept_products(t)
            row_products(t)

        total = jnp.zeros((rows, own_cols), F32)
        squares = jnp.zeros((rows, own_cols), F32)
        for d in NEAR_FIRST:
            local_wait(x.at[t, pl.ds(0, SIDE - 1)], fx_r.at[t, d])
            for e in range(SIDE):
                k = xs(-e) * SIDE + zs(-d)
                block = x[t, k]
                total += jnp.dot(block, w[k], preferred_element_type=F32)
                wide = block.astype(F32)
                squares += wide * wide
        scale = lax.rsqrt(jnp.sum(squares, axis=-1, keepdims=True) / extent + EPSILON)
        result = (x[t, j].astype(F32) + total * scale * inv_root).astype(BF16)
        f_own[t] = result

        @pl.when(t < ticks - 1)
        def _():
            f_send[t] = jnp.where(is_last, inc[jnp.minimum(t, ticks - 2)], result)
            for d in NEAR_LAST:
                remote(
                    f_send.at[t], x.at[t + 1, j], fz_s.at[t + 1], fz_r.at[t + 1, d],
                    (up, r, col * SIDE + zs(d)),
                )
            kept_to_z(t + 1)

        local_wait(p1_in.at[t], p1_r.at[t])
        p2[t] = p1[t] + p1_in[t, 0] + p1_in[t, 1] + p1_in[t, 2]
        for d in NEAR_LAST[:3]:
            remote(
                p2.at[t], p2_in.at[t, d - 1], p2_s.at[t], p2_r.at[t],
                (s, r, col * SIDE + zs(d)),
            )

        local_wait(half_in.at[t], rz_r.at[t])
        branch = keep0[...]
        for d in range(SIDE - 1):
            branch += half_in[t, d].astype(F32)
        local_wait(p2_in.at[t], p2_r.at[t])
        line = p2[t] + p2_in[t, 0] + p2_in[t, 1] + p2_in[t, 2]
        inner = jnp.sum(jnp.where(diagonal, line, 0.0), axis=-1, keepdims=True) / extent
        kept_scale = ks[:, :1]
        hat = kept[j, span, :].astype(F32) * kept_scale
        back = (grad[t].astype(F32) + (branch - hat * inner) * kept_scale).astype(BF16)
        b_own[t] = back

        @pl.when(t < ticks - 1)
        def _():
            b_send[t] = jnp.where(is_first, loss[jnp.minimum(t, ticks - 2)], back)
            remote(b_send.at[t], grad.at[t + 1], g_s.at[t + 1], g_r.at[t + 1], (down, r, j))
            kept_to_x(t + 1)

        return carry

    lax.fori_loop(0, ticks, tick, 0)

    outs = [
        pltpu.make_async_copy(f_own, f_out, out_sem.at[0]),
        pltpu.make_async_copy(b_own, b_out, out_sem.at[1]),
    ]
    for copy in outs:
        copy.start()
    loads[6].wait()
    loads[7].wait()
    for f in range(replicas - 1):
        local_wait(dw_in.at[f], dp_r.at[f])
    for c in range(SIDE):
        summed = dw[r * SIDE + c].astype(F32)
        for f in range(replicas - 1):
            summed += dw_in[f, c].astype(F32)
        velocity = MOMENTUM_RATE * mom[c].astype(F32) + summed
        w_new[c] = (new[c].astype(F32) - LEARNING_RATE * velocity).astype(BF16)
        m_new[c] = velocity.astype(BF16)
    more = [
        pltpu.make_async_copy(w_new, w_out, out_sem.at[2]),
        pltpu.make_async_copy(m_new, m_out, out_sem.at[3]),
    ]
    for copy in more:
        copy.start()

    for t in range(ticks):
        local_wait(x.at[0, pl.ds(0, SIDE if t else SIDE - 1)], fz_s.at[t])
        local_wait(x.at[0, pl.ds(0, SIDE * (SIDE - 1))], fx_s.at[t])
        local_wait(x.at[0, pl.ds(0, SIDE - 1)], kz_s.at[t])
        local_wait(x.at[0, pl.ds(0, SIDE * (SIDE - 1))], kx_s.at[t])
        local_wait(x.at[0, pl.ds(0, SIDE * (SIDE - 1))], rx_s.at[t])
        local_wait(x.at[0, pl.ds(0, SIDE - 1)], rz_s.at[t])
        local_wait(p1_in.at[0], p1_s.at[t])
        local_wait(p2_in.at[0], p2_s.at[t])
        if t:
            local_wait(grad.at[0], g_s.at[t])
    local_wait(dw_in, dp_s)
    for copy in outs + more:
        copy.wait()


def hand_over(f_in, b_in, w_in, m_in, f_out, b_out, w_out, m_out, f, b, w, m, sem):
    pairs = [(f_in, f, f_out), (b_in, b, b_out), (w_in, w, w_out), (m_in, m, m_out)]
    reads = [pltpu.make_async_copy(a, v, sem.at[0, i]) for i, (a, v, _) in enumerate(pairs)]
    writes = [pltpu.make_async_copy(v, o, sem.at[1, i]) for i, (_, v, o) in enumerate(pairs)]
    for copy in reads:
        copy.start()
    for read, write in zip(reads, writes):
        read.wait()
        write.start()
    for copy in writes:
        copy.wait()


def body(
    shadow_weight_copy, newest_weight_version, momentum, pending_section_input,
    incoming_micro_input, pending_output_gradient, loss_gradient_rows, stashed,
):
    extent, cols = shadow_weight_copy.shape[1:]
    ticks, rows = stashed.shape[2:4]
    part_rows = newest_weight_version.shape[1]
    replicas = extent // part_rows
    blocks = extent // cols
    chunk = part_rows // SIDE

    vmem, dma = pltpu.VMEM, pltpu.SemaphoreType.DMA
    block = (rows, cols)
    scratch = [
        vmem((blocks, cols, cols), BF16),
        vmem((ticks, blocks, *block), BF16),
        vmem((blocks, ticks * rows, cols), BF16),
        vmem((ticks, blocks, *block), BF16),
        vmem((ticks, SIDE, SIDE - 1, *block), BF16),
        vmem((ticks, SIDE - 1, *block), BF16),
        vmem((ticks, SIDE - 1, *block), BF16),
        vmem((ticks, *block), BF16),
        vmem((ticks, *block), BF16),
        vmem((ticks, *block), BF16),
        vmem((ticks - 1, *block), BF16),
        vmem((ticks - 1, *block), BF16),
        vmem((ticks - 1, *block), BF16),
        vmem((ticks - 1, *block), BF16),
        vmem((ticks * rows, cols), BF16),
        vmem((ticks, 1, 128), F32),
        vmem((ticks, SIDE - 1, 1, 128), F32),
        vmem((ticks, 1, 128), F32),
        vmem((ticks, SIDE - 1, 1, 128), F32),
        vmem(block, F32),
        vmem((rows, 128), F32),
        vmem(block, F32),
        vmem((blocks, cols, cols), BF16),
        vmem((replicas - 1, SIDE, chunk, cols), BF16),
        vmem((SIDE, chunk, cols), BF16),
        vmem((SIDE, chunk, cols), BF16),
        vmem((SIDE, chunk, cols), BF16),
        vmem((SIDE, chunk, cols), BF16),
        dma((8,)),
        dma((ticks, SIDE)), dma((ticks,)),
        dma((ticks, SIDE)), dma((ticks,)),
        dma((ticks,)), dma((ticks,)),
        dma((ticks,)), dma((ticks,)),
        dma((ticks, SIDE)), dma((ticks,)),
        dma((ticks,)), dma((ticks,)),
        dma((ticks,)), dma((ticks,)),
        dma((ticks,)), dma((ticks,)),
        dma((ticks,)), dma((ticks,)),
        dma((replicas - 1,)), dma,
        dma((4,)),
    ]
    any_space = pl.BlockSpec(memory_space=pl.ANY)
    shape = jax.ShapeDtypeStruct
    f_out, b_out, w_out, m_out = pl.pallas_call(
        kernel,
        name="window",
        out_shape=(
            shape((ticks, *block), BF16),
            shape((ticks, *block), BF16),
            shape((SIDE, chunk, cols), BF16),
            shape((SIDE, chunk, cols), BF16),
        ),
        in_specs=[any_space] * 8,
        out_specs=(any_space,) * 4,
        scratch_shapes=scratch,
        compiler_params=pltpu.CompilerParams(
            collective_id=0, has_side_effects=True, vmem_limit_bytes=60 * 1024 * 1024
        ),
    )(
        shadow_weight_copy.reshape(blocks, cols, cols),
        newest_weight_version.reshape(SIDE, chunk, cols),
        momentum.reshape(SIDE, chunk, cols),
        pending_section_input.reshape(block),
        incoming_micro_input.reshape(ticks - 1, *block),
        pending_output_gradient.reshape(block),
        loss_gradient_rows.reshape(ticks - 1, *block),
        stashed.reshape(ticks * rows, cols),
    )
    f_out, b_out, w_out, m_out = pl.pallas_call(
        hand_over,
        name="hand_over",
        out_shape=(
            shape((ticks, *block), BF16),
            shape((ticks, *block), BF16),
            shape((SIDE, chunk, cols), BF16),
            shape((SIDE, chunk, cols), BF16),
        ),
        in_specs=[any_space] * 4,
        out_specs=(any_space,) * 4,
        scratch_shapes=[
            vmem((ticks, *block), BF16),
            vmem((ticks, *block), BF16),
            vmem((SIDE, chunk, cols), BF16),
            vmem((SIDE, chunk, cols), BF16),
            dma((2, 4)),
        ],
    )(f_out, b_out, w_out, m_out)
    return (
        f_out[None, None],
        b_out[None, None],
        w_out.reshape(1, part_rows, cols),
        m_out.reshape(1, part_rows, cols),
    )


def solution(mesh):
    return jax.shard_map(
        body,
        mesh=mesh,
        in_specs=(
            P("section", None, "tensor"),
            P("section", "dp", "tensor"),
            P("section", "dp", "tensor"),
            P("dp", "section", None, "tensor"),
            P("dp", None, None, "tensor"),
            P("dp", "section", None, "tensor"),
            P("dp", None, None, "tensor"),
            P("dp", "section", None, None, "tensor"),
        ),
        out_specs=(
            P("dp", "section", None, None, "tensor"),
            P("dp", "section", None, None, "tensor"),
            P("section", "dp", "tensor"),
            P("section", "dp", "tensor"),
        ),
        check_vma=False,
    )
```

```python
import functools

import jax
import jax.numpy as jnp
from jax import lax
from jax.experimental import pallas as pl
from jax.experimental.pallas import tpu as pltpu
from jax.sharding import PartitionSpec as P

EPSILON = 1e-06
MOMENTUM_RATE = 0.9
LEARNING_RATE = 0.05
MESH = pl.DeviceIdType.MESH
F32 = jnp.float32
BF16 = jnp.bfloat16

SIDE = 4
NEAR_LAST = (2, 1, 3, 0)
NEAR_FIRST = (0, 1, 3, 2)


def local_wait(ref, sem):
    pltpu.make_async_copy(ref, ref, sem).wait()


def kernel(
    w_in, new_in, mom_in, x_in, inc_in, g_in, loss_in, kept_in,
    f_out, b_out, w_out, m_out,
    w, x, kept, part, part_in, half, half_in, grad, f_own, b_own, f_send, b_send,
    inc, loss, scaled, p1, p1_in, p2, p2_in, kw, ks, keep0, dw, dw_in, new, mom, w_new, m_new,
    load, fz_r, fz_s, fx_r, fx_s, kz_r, kz_s, kx_r, kx_s, rx_r, rx_s, rz_r, rz_s,
    p1_r, p1_s, p2_r, p2_s, g_r, g_s, dp_r, dp_s, out_sem,
):
    blocks, depth, own_cols = w.shape
    ticks, rows = x.shape[0], x.shape[2]
    extent = blocks * depth
    inv_root = 1.0 / float(extent) ** 0.5
    s, r, j = lax.axis_index("section"), lax.axis_index("dp"), lax.axis_index("tensor")
    sections, replicas = lax.axis_size("section"), lax.axis_size("dp")
    col, rank = lax.div(j, SIDE), lax.rem(j, SIDE)
    up, down = lax.rem(s + 1, sections), lax.rem(s + sections - 1, sections)
    is_first, is_last = s == 0, s == sections - 1

    def xs(e):
        return lax.rem(col + e + SIDE, SIDE)

    def zs(d):
        return lax.rem(rank + d + SIDE, SIDE)

    def remote(src, dst, send, recv, device):
        pltpu.make_async_remote_copy(
            src_ref=src, dst_ref=dst, send_sem=send, recv_sem=recv,
            device_id=device, device_id_type=MESH,
        ).start()

    barrier = pltpu.get_barrier_semaphore()
    peers = [(s, r, xs(e) * SIDE + rank) for e in range(1, SIDE)]
    peers += [(s, r, col * SIDE + zs(d)) for d in range(1, SIDE)]
    peers += [(q, r, col * SIDE + zs(d)) for q in (up, down) for d in range(SIDE)]
    peers += [(s, lax.rem(r + f, replicas), j) for f in range(1, replicas)]
    for peer in peers:
        pl.semaphore_signal(barrier, inc=1, device_id=peer, device_id_type=MESH)

    loads = [
        pltpu.make_async_copy(src, dst, load.at[i])
        for i, (src, dst) in enumerate([
            (x_in, x.at[0, j]), (g_in, grad.at[0]), (kept_in, kept.at[j]), (w_in, w),
            (inc_in, inc), (loss_in, loss), (new_in, new), (mom_in, mom),
        ])
    ]
    for copy in loads:
        copy.start()
    for copy in loads[:3]:
        copy.wait()
    pl.semaphore_wait(barrier, len(peers))

    def kept_to_z(t):
        mine = kept.at[j, pl.ds(pl.multiple_of(t * rows, rows), rows), :]
        for d in NEAR_LAST[:3]:
            remote(mine, mine, kz_s.at[t], kz_r.at[t], (s, r, col * SIDE + zs(d)))

    def kept_to_x(t):
        span = pl.ds(pl.multiple_of(t * rows, rows), rows)
        local_wait(kept.at[pl.ds(0, SIDE - 1), span, :], kz_r.at[t])
        group = kept.at[pl.ds(col * SIDE, SIDE), span, :]
        for e in NEAR_LAST[:3]:
            remote(group, group, kx_s.at[t], kx_r.at[t], (s, r, xs(e) * SIDE + rank))

    kept_to_z(0)
    for d in NEAR_LAST[:3]:
        remote(x.at[0, j], x.at[0, j], fz_s.at[0], fz_r.at[0, d], (s, r, col * SIDE + zs(d)))

    loads[3].wait()
    loads[4].wait()
    loads[5].wait()

    row_id = lax.broadcasted_iota(jnp.int32, (rows, 128), 0)
    lane_id = lax.broadcasted_iota(jnp.int32, (rows, 128), 1)
    diagonal = row_id == lane_id

    def kept_products(t):
        span = pl.ds(pl.multiple_of(t * rows, rows), rows)
        local_wait(kept.at[pl.ds(0, SIDE * (SIDE - 1)), span, :], kx_r.at[t])
        product = jnp.zeros((rows, own_cols), F32)
        squares = jnp.zeros((rows, own_cols), F32)
        for k in range(blocks):
            block = kept[k, span, :]
            product += jnp.dot(block, w[k], preferred_element_type=F32)
            wide = block.astype(F32)
            squares += wide * wide
        found = lax.rsqrt(jnp.sum(squares, axis=-1, keepdims=True) / extent + EPSILON)
        kw[...] = product * (found * inv_root)
        ks[...] = jnp.broadcast_to(found, (rows, 128))

    def row_products(t):
        span = pl.ds(pl.multiple_of(t * rows, rows), rows)
        g_wide = grad[t].astype(F32)
        scaled[span, :] = (g_wide * ks[:, :1]).astype(BF16)
        dots = jnp.sum(g_wide * kw[...], axis=-1, keepdims=True)
        p1[t] = jnp.sum(jnp.where(diagonal, dots, 0.0), axis=0, keepdims=True)
        for e in NEAR_LAST[:3]:
            remote(
                p1.at[t], p1_in.at[t, e - 1], p1_s.at[t], p1_r.at[t],
                (s, r, xs(e) * SIDE + rank),
            )

    def row_products_over_x(t):
        local_wait(p1_in.at[t], p1_r.at[t])
        p2[t] = p1[t] + p1_in[t, 0] + p1_in[t, 1] + p1_in[t, 2]
        for d in NEAR_LAST[:3]:
            remote(
                p2.at[t], p2_in.at[t, d - 1], p2_s.at[t], p2_r.at[t],
                (s, r, col * SIDE + zs(d)),
            )

    def tick(t, carry):
        span = pl.ds(pl.multiple_of(t * rows, rows), rows)

        @pl.when(t > 0)
        def _():
            kept_products(t)
            local_wait(grad.at[0], g_r.at[t])
            row_products(t)

        @pl.when(t == ticks - 1)
        def _():
            right = scaled[...]
            for f in (2, 3, 1, 0):
                owner = lax.rem(r + f, replicas)
                for c in range(SIDE):
                    k = owner * SIDE + c
                    term = lax.dot_general(
                        kept[k], right, (((0,), (0,)), ((), ())), preferred_element_type=F32
                    )
                    dw[k] = (term * inv_root).astype(BF16)
                    if f:
                        remote(
                            dw.at[k], dw_in.at[f - 1, c], dp_s, dp_r.at[f - 1], (s, owner, j)
                        )

        g = grad[t]
        for d in NEAR_LAST:
            for e in NEAR_LAST:
                k = xs(e) * SIDE + zs(d)
                term = lax.dot_general(
                    g, w[k], (((1,), (1,)), ((), ())), preferred_element_type=F32
                )
                part[t, k] = (term * inv_root).astype(BF16)
                if e:
                    remote(
                        part.at[t, k], part_in.at[t, d, e - 1], rx_s.at[t], rx_r.at[t, d],
                        (s, r, xs(e) * SIDE + rank),
                    )

        def pass_on(d):
            k = col * SIDE + zs(-d)
            for e in NEAR_LAST[:3]:
                remote(
                    x.at[t, k], x.at[t, k], fx_s.at[t], fx_r.at[t, d],
                    (s, r, xs(e) * SIDE + rank),
                )

        @pl.when(t > 0)
        def _():
            local_wait(x.at[t, 0], fz_r.at[t, 0])

        pass_on(0)

        def over_x(d):
            local_wait(part_in.at[t, d], rx_r.at[t, d])
            total = part[t, col * SIDE + zs(d)].astype(F32)
            for e in range(SIDE - 1):
                total += part_in[t, d, e].astype(F32)
            return total

        for d in (2, 1, 3):
            half[t, d - 1] = over_x(d).astype(BF16)
            remote(
                half.at[t, d - 1], half_in.at[t, d - 1], rz_s.at[t], rz_r.at[t],
                (s, r, col * SIDE + zs(d)),
            )
            if d != 2:
                local_wait(x.at[t, 0], fz_r.at[t, d])
                pass_on(d)
        keep0[...] = over_x(0)

        @pl.when(t == 0)
        def _():
            kept_to_x(0)
            kept_to_z(1)

        local_wait(x.at[t, 0], fz_r.at[t, 2])
        pass_on(2)

        @pl.when(t == 0)
        def _():
            kept_products(0)
            row_products(0)

        @pl.when(t > 0)
        def _():
            row_products_over_x(t)

        @pl.when((t > 0) & (t < ticks - 1))
        def _():
            kept_to_x(t + 1)

        @pl.when((t > 0) & (t < ticks - 2))
        def _():
            kept_to_z(t + 2)

        total = jnp.zeros((rows, own_cols), F32)
        squares = jnp.zeros((rows, own_cols), F32)
        for d in NEAR_FIRST:
            local_wait(x.at[t, pl.ds(0, SIDE - 1)], fx_r.at[t, d])
            for e in range(SIDE):
                k = xs(-e) * SIDE + zs(-d)
                block = x[t, k]
                total += jnp.dot(block, w[k], preferred_element_type=F32)
                wide = block.astype(F32)
                squares += wide * wide
        scale = lax.rsqrt(jnp.sum(squares, axis=-1, keepdims=True) / extent + EPSILON)
        result = (x[t, j].astype(F32) + total * scale * inv_root).astype(BF16)
        f_own[t] = result

        @pl.when(t < ticks - 1)
        def _():
            f_send[t] = jnp.where(is_last, inc[jnp.minimum(t, ticks - 2)], result)
            for d in NEAR_LAST:
                remote(
                    f_send.at[t], x.at[t + 1, j], fz_s.at[t + 1], fz_r.at[t + 1, d],
                    (up, r, col * SIDE + zs(d)),
                )

        @pl.when(t == 0)
        def _():
            row_products_over_x(t)
            kept_to_x(1)
            kept_to_z(2)

        local_wait(half_in.at[t], rz_r.at[t])
        branch = keep0[...]
        for d in range(SIDE - 1):
            branch += half_in[t, d].astype(F32)
        local_wait(p2_in.at[t], p2_r.at[t])
        line = p2[t] + p2_in[t, 0] + p2_in[t, 1] + p2_in[t, 2]
        inner = jnp.sum(jnp.where(diagonal, line, 0.0), axis=-1, keepdims=True) / extent
        kept_scale = ks[:, :1]
        hat = kept[j, span, :].astype(F32) * kept_scale
        back = (grad[t].astype(F32) + (branch - hat * inner) * kept_scale).astype(BF16)
        b_own[t] = back

        @pl.when(t < ticks - 1)
        def _():
            b_send[t] = jnp.where(is_first, loss[jnp.minimum(t, ticks - 2)], back)
            remote(b_send.at[t], grad.at[t + 1], g_s.at[t + 1], g_r.at[t + 1], (down, r, j))

        return carry

    lax.fori_loop(0, ticks, tick, 0)

    outs = [
        pltpu.make_async_copy(f_own, f_out, out_sem.at[0]),
        pltpu.make_async_copy(b_own, b_out, out_sem.at[1]),
    ]
    for copy in outs:
        copy.start()
    loads[6].wait()
    loads[7].wait()
    for f in range(replicas - 1):
        local_wait(dw_in.at[f], dp_r.at[f])
    for c in range(SIDE):
        summed = dw[r * SIDE + c].astype(F32)
        for f in range(replicas - 1):
            summed += dw_in[f, c].astype(F32)
        velocity = MOMENTUM_RATE * mom[c].astype(F32) + summed
        w_new[c] = (new[c].astype(F32) - LEARNING_RATE * velocity).astype(BF16)
        m_new[c] = velocity.astype(BF16)
    more = [
        pltpu.make_async_copy(w_new, w_out, out_sem.at[2]),
        pltpu.make_async_copy(m_new, m_out, out_sem.at[3]),
    ]
    for copy in more:
        copy.start()

    for t in range(ticks):
        local_wait(x.at[0, pl.ds(0, SIDE if t else SIDE - 1)], fz_s.at[t])
        local_wait(x.at[0, pl.ds(0, SIDE * (SIDE - 1))], fx_s.at[t])
        local_wait(x.at[0, pl.ds(0, SIDE - 1)], kz_s.at[t])
        local_wait(x.at[0, pl.ds(0, SIDE * (SIDE - 1))], kx_s.at[t])
        local_wait(x.at[0, pl.ds(0, SIDE * (SIDE - 1))], rx_s.at[t])
        local_wait(x.at[0, pl.ds(0, SIDE - 1)], rz_s.at[t])
        local_wait(p1_in.at[0], p1_s.at[t])
        local_wait(p2_in.at[0], p2_s.at[t])
        if t:
            local_wait(grad.at[0], g_s.at[t])
    local_wait(dw_in, dp_s)
    for copy in outs + more:
        copy.wait()


def hand_over(f_in, b_in, w_in, m_in, f_out, b_out, w_out, m_out, f, b, w, m, sem):
    pairs = [(f_in, f, f_out), (b_in, b, b_out), (w_in, w, w_out), (m_in, m, m_out)]
    reads = [pltpu.make_async_copy(a, v, sem.at[0, i]) for i, (a, v, _) in enumerate(pairs)]
    writes = [pltpu.make_async_copy(v, o, sem.at[1, i]) for i, (_, v, o) in enumerate(pairs)]
    for copy in reads:
        copy.start()
    for read, write in zip(reads, writes):
        read.wait()
        write.start()
    for copy in writes:
        copy.wait()


def body(
    shadow_weight_copy, newest_weight_version, momentum, pending_section_input,
    incoming_micro_input, pending_output_gradient, loss_gradient_rows, stashed,
):
    extent, cols = shadow_weight_copy.shape[1:]
    ticks, rows = stashed.shape[2:4]
    part_rows = newest_weight_version.shape[1]
    replicas = extent // part_rows
    blocks = extent // cols
    chunk = part_rows // SIDE

    vmem, dma = pltpu.VMEM, pltpu.SemaphoreType.DMA
    block = (rows, cols)
    scratch = [
        vmem((blocks, cols, cols), BF16),
        vmem((ticks, blocks, *block), BF16),
        vmem((blocks, ticks * rows, cols), BF16),
        vmem((ticks, blocks, *block), BF16),
        vmem((ticks, SIDE, SIDE - 1, *block), BF16),
        vmem((ticks, SIDE - 1, *block), BF16),
        vmem((ticks, SIDE - 1, *block), BF16),
        vmem((ticks, *block), BF16),
        vmem((ticks, *block), BF16),
        vmem((ticks, *block), BF16),
        vmem((ticks - 1, *block), BF16),
        vmem((ticks - 1, *block), BF16),
        vmem((ticks - 1, *block), BF16),
        vmem((ticks - 1, *block), BF16),
        vmem((ticks * rows, cols), BF16),
        vmem((ticks, 1, 128), F32),
        vmem((ticks, SIDE - 1, 1, 128), F32),
        vmem((ticks, 1, 128), F32),
        vmem((ticks, SIDE - 1, 1, 128), F32),
        vmem(block, F32),
        vmem((rows, 128), F32),
        vmem(block, F32),
        vmem((blocks, cols, cols), BF16),
        vmem((replicas - 1, SIDE, chunk, cols), BF16),
        vmem((SIDE, chunk, cols), BF16),
        vmem((SIDE, chunk, cols), BF16),
        vmem((SIDE, chunk, cols), BF16),
        vmem((SIDE, chunk, cols), BF16),
        dma((8,)),
        dma((ticks, SIDE)), dma((ticks,)),
        dma((ticks, SIDE)), dma((ticks,)),
        dma((ticks,)), dma((ticks,)),
        dma((ticks,)), dma((ticks,)),
        dma((ticks, SIDE)), dma((ticks,)),
        dma((ticks,)), dma((ticks,)),
        dma((ticks,)), dma((ticks,)),
        dma((ticks,)), dma((ticks,)),
        dma((ticks,)), dma((ticks,)),
        dma((replicas - 1,)), dma,
        dma((4,)),
    ]
    any_space = pl.BlockSpec(memory_space=pl.ANY)
    shape = jax.ShapeDtypeStruct
    f_out, b_out, w_out, m_out = pl.pallas_call(
        kernel,
        name="window",
        out_shape=(
            shape((ticks, *block), BF16),
            shape((ticks, *block), BF16),
            shape((SIDE, chunk, cols), BF16),
            shape((SIDE, chunk, cols), BF16),
        ),
        in_specs=[any_space] * 8,
        out_specs=(any_space,) * 4,
        scratch_shapes=scratch,
        compiler_params=pltpu.CompilerParams(
            collective_id=0, has_side_effects=True, vmem_limit_bytes=60 * 1024 * 1024
        ),
    )(
        shadow_weight_copy.reshape(blocks, cols, cols),
        newest_weight_version.reshape(SIDE, chunk, cols),
        momentum.reshape(SIDE, chunk, cols),
        pending_section_input.reshape(block),
        incoming_micro_input.reshape(ticks - 1, *block),
        pending_output_gradient.reshape(block),
        loss_gradient_rows.reshape(ticks - 1, *block),
        stashed.reshape(ticks * rows, cols),
    )
    f_out, b_out, w_out, m_out = pl.pallas_call(
        hand_over,
        name="hand_over",
        out_shape=(
            shape((ticks, *block), BF16),
            shape((ticks, *block), BF16),
            shape((SIDE, chunk, cols), BF16),
            shape((SIDE, chunk, cols), BF16),
        ),
        in_specs=[any_space] * 4,
        out_specs=(any_space,) * 4,
        scratch_shapes=[
            vmem((ticks, *block), BF16),
            vmem((ticks, *block), BF16),
            vmem((SIDE, chunk, cols), BF16),
            vmem((SIDE, chunk, cols), BF16),
            dma((2, 4)),
        ],
    )(f_out, b_out, w_out, m_out)
    return (
        f_out[None, None],
        b_out[None, None],
        w_out.reshape(1, part_rows, cols),
        m_out.reshape(1, part_rows, cols),
    )


def solution(mesh):
    return jax.shard_map(
        body,
        mesh=mesh,
        in_specs=(
            P("section", None, "tensor"),
            P("section", "dp", "tensor"),
            P("section", "dp", "tensor"),
            P("dp", "section", None, "tensor"),
            P("dp", None, None, "tensor"),
            P("dp", "section", None, "tensor"),
            P("dp", None, None, "tensor"),
            P("dp", "section", None, None, "tensor"),
        ),
        out_specs=(
            P("dp", "section", None, None, "tensor"),
            P("dp", "section", None, None, "tensor"),
            P("section", "dp", "tensor"),
            P("section", "dp", "tensor"),
        ),
        check_vma=False,
    )
```

```python
import functools

import jax
import jax.numpy as jnp
from jax import lax
from jax.experimental import pallas as pl
from jax.experimental.pallas import tpu as pltpu
from jax.sharding import PartitionSpec as P

EPSILON = 1e-06
MOMENTUM_RATE = 0.9
LEARNING_RATE = 0.05
MESH = pl.DeviceIdType.MESH
F32 = jnp.float32
BF16 = jnp.bfloat16

SIDE = 4
NEAR_LAST = (2, 1, 3, 0)
NEAR_FIRST = (0, 1, 3, 2)


def local_wait(ref, sem):
    pltpu.make_async_copy(ref, ref, sem).wait()


def kernel(
    w_in, new_in, mom_in, x_in, inc_in, g_in, loss_in, kept_in,
    f_out, b_out, w_out, m_out,
    w, x, kept, part, part_in, half, half_in, grad, f_own, b_own, f_send, b_send,
    inc, loss, scaled, sq, sq_in, dot, dot_in, ks, keep0, rows_all, new, mom, w_new, m_new,
    load, fz_r, fz_s, fx_r, fx_s, kz_r, kz_s, rx_r, rx_s, rz_r, rz_s,
    sq_r, sq_s, dot_r, dot_s, g_r, g_s, sc_r, sc_s, az_r, az_s, ar_r, ar_s, al_r, al_s, out_sem,
):
    blocks, depth, own_cols = w.shape
    ticks, rows = x.shape[0], x.shape[2]
    extent = blocks * depth
    inv_root = 1.0 / float(extent) ** 0.5
    s, r, j = lax.axis_index("section"), lax.axis_index("dp"), lax.axis_index("tensor")
    sections, replicas = lax.axis_size("section"), lax.axis_size("dp")
    col, rank = lax.div(j, SIDE), lax.rem(j, SIDE)
    up, down = lax.rem(s + 1, sections), lax.rem(s + sections - 1, sections)
    is_first, is_last = s == 0, s == sections - 1
    place = lax.rem(col - r + SIDE, SIDE)

    def xs(e):
        return lax.rem(col + e + SIDE, SIDE)

    def zs(d):
        return lax.rem(rank + d + SIDE, SIDE)

    def x_peer(e):
        return (s, r, xs(e) * SIDE + rank)

    def z_peer(d):
        return (s, r, col * SIDE + zs(d))

    def remote(src, dst, send, recv, device):
        pltpu.make_async_remote_copy(
            src_ref=src, dst_ref=dst, send_sem=send, recv_sem=recv,
            device_id=device, device_id_type=MESH,
        ).start()

    barrier = pltpu.get_barrier_semaphore()
    peers = [(s, r, lax.rem(j + i, blocks)) for i in range(1, blocks)]
    peers += [
        (s, lax.rem(r + f, replicas), col * SIDE + zs(d))
        for f in range(1, SIDE) for d in range(SIDE)
    ]
    peers += [(q, r, col * SIDE + zs(d)) for q in (up, down) for d in range(SIDE)]
    for peer in peers:
        pl.semaphore_signal(barrier, inc=1, device_id=peer, device_id_type=MESH)

    loads = [
        pltpu.make_async_copy(src, dst, load.at[i])
        for i, (src, dst) in enumerate([
            (x_in, x.at[0, j]), (kept_in, kept.at[rank]), (g_in, grad.at[0]), (w_in, w),
            (inc_in, inc), (loss_in, loss), (new_in, new), (mom_in, mom),
        ])
    ]
    for copy in loads:
        copy.start()

    row_id = lax.broadcasted_iota(jnp.int32, (rows, 128), 0)
    lane_id = lax.broadcasted_iota(jnp.int32, (rows, 128), 1)
    diagonal = row_id == lane_id

    def to_line(column):
        return jnp.sum(jnp.where(diagonal, column, 0.0), axis=0, keepdims=True)

    def to_column(line):
        return jnp.sum(jnp.where(diagonal, line, 0.0), axis=-1, keepdims=True)

    def share(src, dst_of, send, recv):
        for i in range(1, blocks):
            remote(src, dst_of(i - 1), send, recv, (s, r, lax.rem(j + i, blocks)))

    def span(t):
        return pl.ds(pl.multiple_of(t * rows, rows), rows)

    for copy in loads[:3]:
        copy.wait()
    for t in range(ticks):
        wide = kept[rank, t * rows:(t + 1) * rows, :].astype(F32)
        sq[t] = to_line(jnp.sum(wide * wide, axis=-1, keepdims=True))
    pl.semaphore_wait(barrier, len(peers))

    for d in NEAR_LAST[:3]:
        remote(x.at[0, j], x.at[0, j], fz_s.at[0], fz_r.at[0, d], z_peer(d))

    def kept_to_z(t):
        mine = kept.at[rank, span(t), :]
        for d in NEAR_LAST[:3]:
            remote(mine, mine, kz_s.at[t], kz_r.at[t], z_peer(d))

    kept_to_z(0)
    share(sq, lambda i: sq_in.at[i], sq_s, sq_r)
    for copy in loads[3:6]:
        copy.wait()

    length = kept.shape[1] // 2

    def all_span(h):
        return pl.ds(h * length, length)

    def gather_z(h):
        mine = kept.at[rank, all_span(h), :]
        there = rows_all.at[rank, r, all_span(h), :]
        for d in NEAR_LAST[:3]:
            remote(mine, there, az_s.at[h], az_r.at[h], (s, col, col * SIDE + zs(d)))

        @pl.when(place != 0)
        def _():
            remote(mine, there, az_s.at[h], az_r.at[h], (s, col, j))

        @pl.when(place == 0)
        def _():
            pltpu.make_async_copy(mine, there, az_r.at[h]).start()

    def turn_right(h):
        group = rows_all.at[pl.ds(0, 2), :, all_span(h), :]
        remote(group, group, ar_s.at[h], ar_r.at[h], x_peer(1))

    def turn_left(h):
        group = rows_all.at[pl.ds(2, 2), :, all_span(h), :]
        remote(group, group, al_s.at[h], al_r.at[h], x_peer(-1))

    def wait_right(h):
        local_wait(rows_all.at[pl.ds(0, 2), :, all_span(h), :], ar_r.at[h])

    def wait_left(h):
        local_wait(rows_all.at[pl.ds(2, 2), :, all_span(h), :], al_r.at[h])

    def gather_x1(h):
        @pl.when(place == 0)
        def _():
            local_wait(rows_all.at[:, :, all_span(h), :], az_r.at[h])
            turn_right(h)
            turn_left(h)

    def gather_x2(h):
        @pl.when(place == 1)
        def _():
            wait_right(h)
            turn_right(h)

        @pl.when(place == 3)
        def _():
            wait_left(h)
            turn_left(h)

    def gather_x3(h):
        @pl.when(place == 2)
        def _():
            wait_right(h)
            wait_left(h)
            turn_right(h)
            turn_left(h)

    def gather_end(h):
        @pl.when(place == 1)
        def _():
            wait_left(h)

        @pl.when(place == 3)
        def _():
            wait_right(h)

    def scaled_rows(t):
        scaled[r, span(t), :] = (grad[t].astype(F32) * ks[t, :, :1]).astype(BF16)
        mine = scaled.at[r, span(t), :]
        for f in (2, 1, 3):
            remote(mine, mine, sc_s.at[t], sc_r.at[t], (s, lax.rem(r + f, replicas), j))

    def tick(t, carry):
        @pl.when(t > 0)
        def _():
            local_wait(grad.at[0], g_r.at[t])

        g = grad[t]
        for d in NEAR_LAST:
            for e in NEAR_LAST:
                k = xs(e) * SIDE + zs(d)
                term = lax.dot_general(
                    g, w[k], (((1,), (1,)), ((), ())), preferred_element_type=F32
                )
                part[t, k] = (term * inv_root).astype(BF16)
                if e:
                    remote(
                        part.at[t, k], part_in.at[t, d, e - 1], rx_s.at[t], rx_r.at[t, d],
                        x_peer(e),
                    )

        def pass_on(d):
            k = col * SIDE + zs(-d)
            for e in NEAR_LAST[:3]:
                remote(x.at[t, k], x.at[t, k], fx_s.at[t], fx_r.at[t, d], x_peer(e))

        @pl.when(t > 0)
        def _():
            local_wait(x.at[t, 0], fz_r.at[t, 0])

        pass_on(0)

        local_wait(kept.at[pl.ds(0, SIDE - 1), span(t), :], kz_r.at[t])

        def over_x(d):
            local_wait(part_in.at[t, d], rx_r.at[t, d])
            total = part[t, col * SIDE + zs(d)].astype(F32)
            for e in range(SIDE - 1):
                total += part_in[t, d, e].astype(F32)
            return total

        products = jnp.zeros((rows, own_cols), F32)
        for d in (2, 1, 3):
            total = over_x(d)
            half[t, d - 1] = total.astype(BF16)
            remote(half.at[t, d - 1], half_in.at[t, d - 1], rz_s.at[t], rz_r.at[t], z_peer(d))
            products += total * kept[zs(d), span(t), :].astype(F32)
            if d != 2:
                local_wait(x.at[t, 0], fz_r.at[t, d])
                pass_on(d)
        total = over_x(0)
        keep0[...] = total
        products += total * kept[rank, span(t), :].astype(F32)
        dot[t] = to_line(jnp.sum(products, axis=-1, keepdims=True))
        share(dot.at[t], lambda i: dot_in.at[t, i], dot_s.at[t], dot_r.at[t])

        local_wait(x.at[t, 0], fz_r.at[t, 2])
        pass_on(2)

        @pl.when(t < ticks - 1)
        def _():
            kept_to_z(t + 1)

        @pl.when(t == 0)
        def _():
            gather_z(0)

        @pl.when(t == 1)
        def _():
            gather_x1(0)

        @pl.when(t == 2)
        def _():
            gather_x2(0)

        @pl.when(t == 3)
        def _():
            scaled_rows(t)
            gather_x3(0)
            gather_x3(1)

        total = jnp.zeros((rows, own_cols), F32)
        squares = jnp.zeros((rows, own_cols), F32)
        for d in NEAR_FIRST:
            local_wait(x.at[t, pl.ds(0, SIDE - 1)], fx_r.at[t, d])
            for e in range(SIDE):
                k = xs(-e) * SIDE + zs(-d)
                block = x[t, k]
                total += jnp.dot(block, w[k], preferred_element_type=F32)
                wide = block.astype(F32)
                squares += wide * wide
        scale = lax.rsqrt(jnp.sum(squares, axis=-1, keepdims=True) / extent + EPSILON)
        result = (x[t, j].astype(F32) + total * scale * inv_root).astype(BF16)
        f_own[t] = result

        @pl.when(t < ticks - 1)
        def _():
            f_send[t] = jnp.where(is_last, inc[jnp.minimum(t, ticks - 2)], result)
            for d in NEAR_LAST:
                remote(
                    f_send.at[t], x.at[t + 1, j], fz_s.at[t + 1], fz_r.at[t + 1, d],
                    (up, r, col * SIDE + zs(d)),
                )

        @pl.when(t == 0)
        def _():
            gather_z(1)
            local_wait(sq_in, sq_r)
            lines = sq[...] + jnp.sum(sq_in[...], axis=0)
            for u in range(ticks):
                found = lax.rsqrt(to_column(lines[u]) / extent + EPSILON)
                ks[u] = jnp.broadcast_to(found, (rows, 128))

        @pl.when(t < ticks - 1)
        def _():
            scaled_rows(t)

        @pl.when(t == 1)
        def _():
            gather_x1(1)

        @pl.when(t == 2)
        def _():
            gather_x2(1)

        local_wait(half_in.at[t], rz_r.at[t])
        branch = keep0[...]
        for d in range(SIDE - 1):
            branch += half_in[t, d].astype(F32)
        local_wait(dot_in.at[t], dot_r.at[t])
        kept_scale = ks[t, :, :1]
        inner = to_column(dot[t] + jnp.sum(dot_in[t], axis=0)) * kept_scale / extent
        hat = kept[rank, span(t), :].astype(F32) * kept_scale
        back = (grad[t].astype(F32) + (branch - hat * inner) * kept_scale).astype(BF16)
        b_own[t] = back

        @pl.when(t < ticks - 1)
        def _():
            b_send[t] = jnp.where(is_first, loss[jnp.minimum(t, ticks - 2)], back)
            remote(b_send.at[t], grad.at[t + 1], g_s.at[t + 1], g_r.at[t + 1], (down, r, j))

        return carry

    lax.fori_loop(0, ticks, tick, 0)

    outs = [
        pltpu.make_async_copy(f_own, f_out, out_sem.at[0]),
        pltpu.make_async_copy(b_own, b_out, out_sem.at[1]),
    ]
    for copy in outs:
        copy.start()
    loads[6].wait()
    loads[7].wait()
    for t in range(ticks):
        local_wait(scaled.at[pl.ds(0, SIDE - 1), span(t), :], sc_r.at[t])
    gather_end(0)
    gather_end(1)
    for c in range(SIDE):
        summed = jnp.zeros((depth, own_cols), F32)
        for q in range(SIDE):
            summed += lax.dot_general(
                rows_all[c, q], scaled[q], (((0,), (0,)), ((), ())), preferred_element_type=F32
            )
        velocity = MOMENTUM_RATE * mom[c].astype(F32) + summed * inv_root
        w_new[c] = (new[c].astype(F32) - LEARNING_RATE * velocity).astype(BF16)
        m_new[c] = velocity.astype(BF16)
    more = [
        pltpu.make_async_copy(w_new, w_out, out_sem.at[2]),
        pltpu.make_async_copy(m_new, m_out, out_sem.at[3]),
    ]
    for copy in more:
        copy.start()

    local_wait(sq_in, sq_s)
    for t in range(ticks):
        local_wait(x.at[0, pl.ds(0, SIDE if t else SIDE - 1)], fz_s.at[t])
        local_wait(x.at[0, pl.ds(0, SIDE * (SIDE - 1))], fx_s.at[t])
        local_wait(x.at[0, pl.ds(0, SIDE - 1)], kz_s.at[t])
        local_wait(x.at[0, pl.ds(0, SIDE * (SIDE - 1))], rx_s.at[t])
        local_wait(x.at[0, pl.ds(0, SIDE - 1)], rz_s.at[t])
        local_wait(x.at[0, pl.ds(0, SIDE - 1)], sc_s.at[t])
        local_wait(dot_in.at[0], dot_s.at[t])
        if t:
            local_wait(grad.at[0], g_s.at[t])
    for h in range(2):
        local_wait(rows_all.at[0, pl.ds(0, SIDE - 1), all_span(h), :], az_s.at[h])

        @pl.when(place != 0)
        def _():
            local_wait(rows_all.at[0, 0, all_span(h), :], az_s.at[h])

        @pl.when(place != 3)
        def _():
            local_wait(rows_all.at[pl.ds(0, 2), :, all_span(h), :], ar_s.at[h])

        @pl.when(place != 1)
        def _():
            local_wait(rows_all.at[pl.ds(2, 2), :, all_span(h), :], al_s.at[h])

    for copy in outs + more:
        copy.wait()


def hand_over(f_in, b_in, w_in, m_in, f_out, b_out, w_out, m_out, f, b, w, m, sem):
    pairs = [(f_in, f, f_out), (b_in, b, b_out), (w_in, w, w_out), (m_in, m, m_out)]
    reads = [pltpu.make_async_copy(a, v, sem.at[0, i]) for i, (a, v, _) in enumerate(pairs)]
    writes = [pltpu.make_async_copy(v, o, sem.at[1, i]) for i, (_, v, o) in enumerate(pairs)]
    for copy in reads:
        copy.start()
    for read, write in zip(reads, writes):
        read.wait()
        write.start()
    for copy in writes:
        copy.wait()


def body(
    shadow_weight_copy, newest_weight_version, momentum, pending_section_input,
    incoming_micro_input, pending_output_gradient, loss_gradient_rows, stashed,
):
    extent, cols = shadow_weight_copy.shape[1:]
    ticks, rows = stashed.shape[2:4]
    part_rows = newest_weight_version.shape[1]
    replicas = extent // part_rows
    blocks = extent // cols
    chunk = part_rows // SIDE

    vmem, dma = pltpu.VMEM, pltpu.SemaphoreType.DMA
    block = (rows, cols)
    scratch = [
        vmem((blocks, cols, cols), BF16),
        vmem((ticks, blocks, *block), BF16),
        vmem((SIDE, ticks * rows, cols), BF16),
        vmem((ticks, blocks, *block), BF16),
        vmem((ticks, SIDE, SIDE - 1, *block), BF16),
        vmem((ticks, SIDE - 1, *block), BF16),
        vmem((ticks, SIDE - 1, *block), BF16),
        vmem((ticks, *block), BF16),
        vmem((ticks, *block), BF16),
        vmem((ticks, *block), BF16),
        vmem((ticks - 1, *block), BF16),
        vmem((ticks - 1, *block), BF16),
        vmem((ticks - 1, *block), BF16),
        vmem((ticks - 1, *block), BF16),
        vmem((replicas, ticks * rows, cols), BF16),
        vmem((ticks, 1, 128), F32),
        vmem((blocks - 1, ticks, 1, 128), F32),
        vmem((ticks, 1, 128), F32),
        vmem((ticks, blocks - 1, 1, 128), F32),
        vmem((ticks, rows, 128), F32),
        vmem(block, F32),
        vmem((SIDE, replicas, ticks * rows, cols), BF16),
        vmem((SIDE, chunk, cols), BF16),
        vmem((SIDE, chunk, cols), BF16),
        vmem((SIDE, chunk, cols), BF16),
        vmem((SIDE, chunk, cols), BF16),
        dma((8,)),
        dma((ticks, SIDE)), dma((ticks,)),
        dma((ticks, SIDE)), dma((ticks,)),
        dma((ticks,)), dma((ticks,)),
        dma((ticks, SIDE)), dma((ticks,)),
        dma((ticks,)), dma((ticks,)),
        dma, dma,
        dma((ticks,)), dma((ticks,)),
        dma((ticks,)), dma((ticks,)),
        dma((ticks,)), dma((ticks,)),
        dma((2,)), dma((2,)),
        dma((2,)), dma((2,)),
        dma((2,)), dma((2,)),
        dma((4,)),
    ]
    any_space = pl.BlockSpec(memory_space=pl.ANY)
    shape = jax.ShapeDtypeStruct
    f_out, b_out, w_out, m_out = pl.pallas_call(
        kernel,
        name="window",
        out_shape=(
            shape((ticks, *block), BF16),
            shape((ticks, *block), BF16),
            shape((SIDE, chunk, cols), BF16),
            shape((SIDE, chunk, cols), BF16),
        ),
        in_specs=[any_space] * 8,
        out_specs=(any_space,) * 4,
        scratch_shapes=scratch,
        compiler_params=pltpu.CompilerParams(
            collective_id=0, has_side_effects=True, vmem_limit_bytes=60 * 1024 * 1024
        ),
    )(
        shadow_weight_copy.reshape(blocks, cols, cols),
        newest_weight_version.reshape(SIDE, chunk, cols),
        momentum.reshape(SIDE, chunk, cols),
        pending_section_input.reshape(block),
        incoming_micro_input.reshape(ticks - 1, *block),
        pending_output_gradient.reshape(block),
        loss_gradient_rows.reshape(ticks - 1, *block),
        stashed.reshape(ticks * rows, cols),
    )
    f_out, b_out, w_out, m_out = pl.pallas_call(
        hand_over,
        name="hand_over",
        out_shape=(
            shape((ticks, *block), BF16),
            shape((ticks, *block), BF16),
            shape((SIDE, chunk, cols), BF16),
            shape((SIDE, chunk, cols), BF16),
        ),
        in_specs=[any_space] * 4,
        out_specs=(any_space,) * 4,
        scratch_shapes=[
            vmem((ticks, *block), BF16),
            vmem((ticks, *block), BF16),
            vmem((SIDE, chunk, cols), BF16),
            vmem((SIDE, chunk, cols), BF16),
            dma((2, 4)),
        ],
    )(f_out, b_out, w_out, m_out)
    return (
        f_out[None, None],
        b_out[None, None],
        w_out.reshape(1, part_rows, cols),
        m_out.reshape(1, part_rows, cols),
    )


def solution(mesh):
    return jax.shard_map(
        body,
        mesh=mesh,
        in_specs=(
            P("section", None, "tensor"),
            P("section", "dp", "tensor"),
            P("section", "dp", "tensor"),
            P("dp", "section", None, "tensor"),
            P("dp", None, None, "tensor"),
            P("dp", "section", None, "tensor"),
            P("dp", None, None, "tensor"),
            P("dp", "section", None, None, "tensor"),
        ),
        out_specs=(
            P("dp", "section", None, None, "tensor"),
            P("dp", "section", None, None, "tensor"),
            P("section", "dp", "tensor"),
            P("section", "dp", "tensor"),
        ),
        check_vma=False,
    )
```

```python
import functools

import jax
import jax.numpy as jnp
from jax import lax
from jax.experimental import pallas as pl
from jax.experimental.pallas import tpu as pltpu
from jax.sharding import PartitionSpec as P

EPSILON = 1e-06
MOMENTUM_RATE = 0.9
LEARNING_RATE = 0.05
MESH = pl.DeviceIdType.MESH
F32 = jnp.float32
BF16 = jnp.bfloat16

SIDE = 4
NEAR_LAST = (2, 1, 3, 0)
NEAR_FIRST = (0, 1, 3, 2)


def local_wait(ref, sem):
    pltpu.make_async_copy(ref, ref, sem).wait()


def kernel(
    w_in, new_in, mom_in, x_in, inc_in, g_in, loss_in, kept_in,
    f_out, b_out, w_out, m_out,
    w, x, kept, part, part_in, half, half_in, grad, f_own, b_own, f_send, b_send,
    inc, loss, scaled, p1, p1_in, p2, p2_in, kw, ks, keep0, dw, dw_in, own_sum, kept_pair, scaled_pair, new, mom, w_new, m_new,
    load, fz_r, fz_s, fx_r, fx_s, kz_r, kz_s, kx_r, kx_s, rx_r, rx_s, rz_r, rz_s,
    p1_r, p1_s, p2_r, p2_s, g_r, g_s, pk_r, pk_s, ps_r, ps_s, dp_r, dp_s, out_sem,
):
    blocks, depth, own_cols = w.shape
    ticks, rows = x.shape[0], x.shape[2]
    extent = blocks * depth
    inv_root = 1.0 / float(extent) ** 0.5
    s, r, j = lax.axis_index("section"), lax.axis_index("dp"), lax.axis_index("tensor")
    sections, replicas = lax.axis_size("section"), lax.axis_size("dp")
    col, rank = lax.div(j, SIDE), lax.rem(j, SIDE)
    up, down = lax.rem(s + 1, sections), lax.rem(s + sections - 1, sections)
    is_first, is_last = s == 0, s == sections - 1
    pair = r + 1 - 2 * lax.rem(r, 2)
    far = lax.rem(r + 2, replicas)
    beyond = lax.rem(pair + 2, replicas)

    def xs(e):
        return lax.rem(col + e + SIDE, SIDE)

    def zs(d):
        return lax.rem(rank + d + SIDE, SIDE)

    def remote(src, dst, send, recv, device):
        pltpu.make_async_remote_copy(
            src_ref=src, dst_ref=dst, send_sem=send, recv_sem=recv,
            device_id=device, device_id_type=MESH,
        ).start()

    barrier = pltpu.get_barrier_semaphore()
    peers = [(s, r, xs(e) * SIDE + rank) for e in range(1, SIDE)]
    peers += [(s, r, col * SIDE + zs(d)) for d in range(1, SIDE)]
    peers += [(q, r, col * SIDE + zs(d)) for q in (up, down) for d in range(SIDE)]
    peers += [(s, lax.rem(r + f, replicas), j) for f in range(1, replicas)]
    for peer in peers:
        pl.semaphore_signal(barrier, inc=1, device_id=peer, device_id_type=MESH)

    loads = [
        pltpu.make_async_copy(src, dst, load.at[i])
        for i, (src, dst) in enumerate([
            (x_in, x.at[0, j]), (g_in, grad.at[0]), (kept_in, kept.at[j]), (w_in, w),
            (inc_in, inc), (loss_in, loss), (new_in, new), (mom_in, mom),
        ])
    ]
    for copy in loads:
        copy.start()
    for copy in loads[:3]:
        copy.wait()
    pl.semaphore_wait(barrier, len(peers))

    def kept_to_z(t):
        mine = kept.at[j, pl.ds(pl.multiple_of(t * rows, rows), rows), :]
        for d in NEAR_LAST[:3]:
            remote(mine, mine, kz_s.at[t], kz_r.at[t], (s, r, col * SIDE + zs(d)))

    def kept_to_x(t):
        span = pl.ds(pl.multiple_of(t * rows, rows), rows)
        local_wait(kept.at[pl.ds(0, SIDE - 1), span, :], kz_r.at[t])
        group = kept.at[pl.ds(col * SIDE, SIDE), span, :]
        for e in NEAR_LAST[:3]:
            remote(group, group, kx_s.at[t], kx_r.at[t], (s, r, xs(e) * SIDE + rank))

    kept_to_z(0)
    for d in NEAR_LAST[:3]:
        remote(x.at[0, j], x.at[0, j], fz_s.at[0], fz_r.at[0, d], (s, r, col * SIDE + zs(d)))

    loads[3].wait()
    loads[4].wait()
    loads[5].wait()

    row_id = lax.broadcasted_iota(jnp.int32, (rows, 128), 0)
    lane_id = lax.broadcasted_iota(jnp.int32, (rows, 128), 1)
    diagonal = row_id == lane_id

    def kept_products(t):
        span = pl.ds(pl.multiple_of(t * rows, rows), rows)
        local_wait(kept.at[pl.ds(0, SIDE * (SIDE - 1)), span, :], kx_r.at[t])
        for i, owner in ((1, beyond), (0, pair)):
            remote(
                kept.at[pl.ds(owner * SIDE, SIDE), span, :], kept_pair.at[i, :, span, :],
                pk_s.at[t], pk_r.at[t], (s, pair, j),
            )
        product = jnp.zeros((rows, own_cols), F32)
        squares = jnp.zeros((rows, own_cols), F32)
        for k in range(blocks):
            block = kept[k, span, :]
            product += jnp.dot(block, w[k], preferred_element_type=F32)
            wide = block.astype(F32)
            squares += wide * wide
        found = lax.rsqrt(jnp.sum(squares, axis=-1, keepdims=True) / extent + EPSILON)
        kw[...] = product * (found * inv_root)
        ks[...] = jnp.broadcast_to(found, (rows, 128))

    def row_products(t):
        span = pl.ds(pl.multiple_of(t * rows, rows), rows)
        g_wide = grad[t].astype(F32)
        scaled[span, :] = (g_wide * ks[:, :1]).astype(BF16)
        remote(
            scaled.at[span, :], scaled_pair.at[span, :], ps_s.at[t], ps_r.at[t], (s, pair, j)
        )
        dots = jnp.sum(g_wide * kw[...], axis=-1, keepdims=True)
        p1[t] = jnp.sum(jnp.where(diagonal, dots, 0.0), axis=0, keepdims=True)
        for e in NEAR_LAST[:3]:
            remote(
                p1.at[t], p1_in.at[t, e - 1], p1_s.at[t], p1_r.at[t],
                (s, r, xs(e) * SIDE + rank),
            )

    def row_products_over_x(t):
        local_wait(p1_in.at[t], p1_r.at[t])
        p2[t] = p1[t] + p1_in[t, 0] + p1_in[t, 1] + p1_in[t, 2]
        for d in NEAR_LAST[:3]:
            remote(
                p2.at[t], p2_in.at[t, d - 1], p2_s.at[t], p2_r.at[t],
                (s, r, col * SIDE + zs(d)),
            )

    def pair_gradient(owner, i, c):
        over_rows = (((0,), (0,)), ((), ()))
        term = lax.dot_general(
            kept[owner * SIDE + c], scaled[...], over_rows, preferred_element_type=F32
        )
        term += lax.dot_general(
            kept_pair[i, c], scaled_pair[...], over_rows, preferred_element_type=F32
        )
        return term * inv_root

    def tick(t, carry):
        span = pl.ds(pl.multiple_of(t * rows, rows), rows)

        @pl.when(t > 0)
        def _():
            kept_products(t)
            local_wait(grad.at[0], g_r.at[t])
            row_products(t)

        g = grad[t]
        for d in NEAR_LAST:
            for e in NEAR_LAST:
                k = xs(e) * SIDE + zs(d)
                term = lax.dot_general(
                    g, w[k], (((1,), (1,)), ((), ())), preferred_element_type=F32
                )
                part[t, k] = (term * inv_root).astype(BF16)
                if e:
                    remote(
                        part.at[t, k], part_in.at[t, d, e - 1], rx_s.at[t], rx_r.at[t, d],
                        (s, r, xs(e) * SIDE + rank),
                    )

        def pass_on(d):
            k = col * SIDE + zs(-d)
            for e in NEAR_LAST[:3]:
                remote(
                    x.at[t, k], x.at[t, k], fx_s.at[t], fx_r.at[t, d],
                    (s, r, xs(e) * SIDE + rank),
                )

        @pl.when(t > 0)
        def _():
            local_wait(x.at[t, 0], fz_r.at[t, 0])

        pass_on(0)

        @pl.when(t == ticks - 1)
        def _():
            for u in range(ticks):
                rows_u = pl.ds(u * rows, rows)
                local_wait(kept_pair.at[:, :, rows_u, :], pk_r.at[u])
                local_wait(scaled_pair.at[rows_u, :], ps_r.at[u])
            for c in range(SIDE):
                dw[c] = pair_gradient(far, 1, c).astype(BF16)
                remote(dw.at[c], dw_in.at[c], dp_s, dp_r, (s, far, j))

        def over_x(d):
            local_wait(part_in.at[t, d], rx_r.at[t, d])
            total = part[t, col * SIDE + zs(d)].astype(F32)
            for e in range(SIDE - 1):
                total += part_in[t, d, e].astype(F32)
            return total

        for d in (2, 1, 3):
            half[t, d - 1] = over_x(d).astype(BF16)
            remote(
                half.at[t, d - 1], half_in.at[t, d - 1], rz_s.at[t], rz_r.at[t],
                (s, r, col * SIDE + zs(d)),
            )
            if d != 2:
                local_wait(x.at[t, 0], fz_r.at[t, d])
                pass_on(d)
        keep0[...] = over_x(0)

        @pl.when(t == 0)
        def _():
            kept_to_x(0)
            kept_to_z(1)

        local_wait(x.at[t, 0], fz_r.at[t, 2])
        pass_on(2)

        @pl.when(t == 0)
        def _():
            kept_products(0)
            row_products(0)

        @pl.when(t > 0)
        def _():
            row_products_over_x(t)

        @pl.when((t > 0) & (t < ticks - 1))
        def _():
            kept_to_x(t + 1)

        @pl.when((t > 0) & (t < ticks - 2))
        def _():
            kept_to_z(t + 2)

        total = jnp.zeros((rows, own_cols), F32)
        squares = jnp.zeros((rows, own_cols), F32)
        for d in NEAR_FIRST:
            local_wait(x.at[t, pl.ds(0, SIDE - 1)], fx_r.at[t, d])
            for e in range(SIDE):
                k = xs(-e) * SIDE + zs(-d)
                block = x[t, k]
                total += jnp.dot(block, w[k], preferred_element_type=F32)
                wide = block.astype(F32)
                squares += wide * wide
        scale = lax.rsqrt(jnp.sum(squares, axis=-1, keepdims=True) / extent + EPSILON)
        result = (x[t, j].astype(F32) + total * scale * inv_root).astype(BF16)
        f_own[t] = result

        @pl.when(t < ticks - 1)
        def _():
            f_send[t] = jnp.where(is_last, inc[jnp.minimum(t, ticks - 2)], result)
            for d in NEAR_LAST:
                remote(
                    f_send.at[t], x.at[t + 1, j], fz_s.at[t + 1], fz_r.at[t + 1, d],
                    (up, r, col * SIDE + zs(d)),
                )

        @pl.when(t == 0)
        def _():
            row_products_over_x(t)
            kept_to_x(1)
            kept_to_z(2)

        local_wait(half_in.at[t], rz_r.at[t])
        branch = keep0[...]
        for d in range(SIDE - 1):
            branch += half_in[t, d].astype(F32)
        local_wait(p2_in.at[t], p2_r.at[t])
        line = p2[t] + p2_in[t, 0] + p2_in[t, 1] + p2_in[t, 2]
        inner = jnp.sum(jnp.where(diagonal, line, 0.0), axis=-1, keepdims=True) / extent
        kept_scale = ks[:, :1]
        hat = kept[j, span, :].astype(F32) * kept_scale
        back = (grad[t].astype(F32) + (branch - hat * inner) * kept_scale).astype(BF16)
        b_own[t] = back

        @pl.when(t < ticks - 1)
        def _():
            b_send[t] = jnp.where(is_first, loss[jnp.minimum(t, ticks - 2)], back)
            remote(b_send.at[t], grad.at[t + 1], g_s.at[t + 1], g_r.at[t + 1], (down, r, j))

        return carry

    lax.fori_loop(0, ticks, tick, 0)

    outs = [
        pltpu.make_async_copy(f_own, f_out, out_sem.at[0]),
        pltpu.make_async_copy(b_own, b_out, out_sem.at[1]),
    ]
    for copy in outs:
        copy.start()
    loads[6].wait()
    loads[7].wait()
    for c in range(SIDE):
        own_sum[c] = pair_gradient(r, 0, c)
    local_wait(dw_in, dp_r)
    for c in range(SIDE):
        summed = own_sum[c] + dw_in[c].astype(F32)
        velocity = MOMENTUM_RATE * mom[c].astype(F32) + summed
        w_new[c] = (new[c].astype(F32) - LEARNING_RATE * velocity).astype(BF16)
        m_new[c] = velocity.astype(BF16)
    more = [
        pltpu.make_async_copy(w_new, w_out, out_sem.at[2]),
        pltpu.make_async_copy(m_new, m_out, out_sem.at[3]),
    ]
    for copy in more:
        copy.start()

    for t in range(ticks):
        local_wait(x.at[0, pl.ds(0, SIDE if t else SIDE - 1)], fz_s.at[t])
        local_wait(x.at[0, pl.ds(0, SIDE * (SIDE - 1))], fx_s.at[t])
        local_wait(x.at[0, pl.ds(0, SIDE - 1)], kz_s.at[t])
        local_wait(x.at[0, pl.ds(0, SIDE * (SIDE - 1))], kx_s.at[t])
        local_wait(x.at[0, pl.ds(0, SIDE * (SIDE - 1))], rx_s.at[t])
        local_wait(x.at[0, pl.ds(0, SIDE - 1)], rz_s.at[t])
        local_wait(p1_in.at[0], p1_s.at[t])
        local_wait(p2_in.at[0], p2_s.at[t])
        local_wait(x.at[0, pl.ds(0, 2 * SIDE)], pk_s.at[t])
        local_wait(grad.at[0], ps_s.at[t])
        if t:
            local_wait(grad.at[0], g_s.at[t])
    local_wait(dw, dp_s)
    for copy in outs + more:
        copy.wait()


def hand_over(f_in, b_in, w_in, m_in, f_out, b_out, w_out, m_out, f, b, w, m, sem):
    pairs = [(f_in, f, f_out), (b_in, b, b_out), (w_in, w, w_out), (m_in, m, m_out)]
    reads = [pltpu.make_async_copy(a, v, sem.at[0, i]) for i, (a, v, _) in enumerate(pairs)]
    writes = [pltpu.make_async_copy(v, o, sem.at[1, i]) for i, (_, v, o) in enumerate(pairs)]
    for copy in reads:
        copy.start()
    for read, write in zip(reads, writes):
        read.wait()
        write.start()
    for copy in writes:
        copy.wait()


def body(
    shadow_weight_copy, newest_weight_version, momentum, pending_section_input,
    incoming_micro_input, pending_output_gradient, loss_gradient_rows, stashed,
):
    extent, cols = shadow_weight_copy.shape[1:]
    ticks, rows = stashed.shape[2:4]
    part_rows = newest_weight_version.shape[1]
    replicas = extent // part_rows
    blocks = extent // cols
    chunk = part_rows // SIDE

    vmem, dma = pltpu.VMEM, pltpu.SemaphoreType.DMA
    block = (rows, cols)
    scratch = [
        vmem((blocks, cols, cols), BF16),
        vmem((ticks, blocks, *block), BF16),
        vmem((blocks, ticks * rows, cols), BF16),
        vmem((ticks, blocks, *block), BF16),
        vmem((ticks, SIDE, SIDE - 1, *block), BF16),
        vmem((ticks, SIDE - 1, *block), BF16),
        vmem((ticks, SIDE - 1, *block), BF16),
        vmem((ticks, *block), BF16),
        vmem((ticks, *block), BF16),
        vmem((ticks, *block), BF16),
        vmem((ticks - 1, *block), BF16),
        vmem((ticks - 1, *block), BF16),
        vmem((ticks - 1, *block), BF16),
        vmem((ticks - 1, *block), BF16),
        vmem((ticks * rows, cols), BF16),
        vmem((ticks, 1, 128), F32),
        vmem((ticks, SIDE - 1, 1, 128), F32),
        vmem((ticks, 1, 128), F32),
        vmem((ticks, SIDE - 1, 1, 128), F32),
        vmem(block, F32),
        vmem((rows, 128), F32),
        vmem(block, F32),
        vmem((SIDE, chunk, cols), BF16),
        vmem((SIDE, chunk, cols), BF16),
        vmem((SIDE, chunk, cols), F32),
        vmem((2, SIDE, ticks * rows, cols), BF16),
        vmem((ticks * rows, cols), BF16),
        vmem((SIDE, chunk, cols), BF16),
        vmem((SIDE, chunk, cols), BF16),
        vmem((SIDE, chunk, cols), BF16),
        vmem((SIDE, chunk, cols), BF16),
        dma((8,)),
        dma((ticks, SIDE)), dma((ticks,)),
        dma((ticks, SIDE)), dma((ticks,)),
        dma((ticks,)), dma((ticks,)),
        dma((ticks,)), dma((ticks,)),
        dma((ticks, SIDE)), dma((ticks,)),
        dma((ticks,)), dma((ticks,)),
        dma((ticks,)), dma((ticks,)),
        dma((ticks,)), dma((ticks,)),
        dma((ticks,)), dma((ticks,)),
        dma((ticks,)), dma((ticks,)),
        dma((ticks,)), dma((ticks,)),
        dma, dma,
        dma((4,)),
    ]
    any_space = pl.BlockSpec(memory_space=pl.ANY)
    shape = jax.ShapeDtypeStruct
    f_out, b_out, w_out, m_out = pl.pallas_call(
        kernel,
        name="window",
        out_shape=(
            shape((ticks, *block), BF16),
            shape((ticks, *block), BF16),
            shape((SIDE, chunk, cols), BF16),
            shape((SIDE, chunk, cols), BF16),
        ),
        in_specs=[any_space] * 8,
        out_specs=(any_space,) * 4,
        scratch_shapes=scratch,
        compiler_params=pltpu.CompilerParams(
            collective_id=0, has_side_effects=True, vmem_limit_bytes=60 * 1024 * 1024
        ),
    )(
        shadow_weight_copy.reshape(blocks, cols, cols),
        newest_weight_version.reshape(SIDE, chunk, cols),
        momentum.reshape(SIDE, chunk, cols),
        pending_section_input.reshape(block),
        incoming_micro_input.reshape(ticks - 1, *block),
        pending_output_gradient.reshape(block),
        loss_gradient_rows.reshape(ticks - 1, *block),
        stashed.reshape(ticks * rows, cols),
    )
    f_out, b_out, w_out, m_out = pl.pallas_call(
        hand_over,
        name="hand_over",
        out_shape=(
            shape((ticks, *block), BF16),
            shape((ticks, *block), BF16),
            shape((SIDE, chunk, cols), BF16),
            shape((SIDE, chunk, cols), BF16),
        ),
        in_specs=[any_space] * 4,
        out_specs=(any_space,) * 4,
        scratch_shapes=[
            vmem((ticks, *block), BF16),
            vmem((ticks, *block), BF16),
            vmem((SIDE, chunk, cols), BF16),
            vmem((SIDE, chunk, cols), BF16),
            dma((2, 4)),
        ],
    )(f_out, b_out, w_out, m_out)
    return (
        f_out[None, None],
        b_out[None, None],
        w_out.reshape(1, part_rows, cols),
        m_out.reshape(1, part_rows, cols),
    )


def solution(mesh):
    return jax.shard_map(
        body,
        mesh=mesh,
        in_specs=(
            P("section", None, "tensor"),
            P("section", "dp", "tensor"),
            P("section", "dp", "tensor"),
            P("dp", "section", None, "tensor"),
            P("dp", None, None, "tensor"),
            P("dp", "section", None, "tensor"),
            P("dp", None, None, "tensor"),
            P("dp", "section", None, None, "tensor"),
        ),
        out_specs=(
            P("dp", "section", None, None, "tensor"),
            P("dp", "section", None, None, "tensor"),
            P("section", "dp", "tensor"),
            P("section", "dp", "tensor"),
        ),
        check_vma=False,
    )
```

```python
import functools

import jax
import jax.numpy as jnp
from jax import lax
from jax.experimental import pallas as pl
from jax.experimental.pallas import tpu as pltpu
from jax.sharding import PartitionSpec as P

EPSILON = 1e-06
MOMENTUM_RATE = 0.9
LEARNING_RATE = 0.05
MESH = pl.DeviceIdType.MESH
F32 = jnp.float32
BF16 = jnp.bfloat16

SIDE = 4
NEAR_LAST = (2, 1, 3, 0)
NEAR_FIRST = (0, 1, 3, 2)


def local_wait(ref, sem):
    pltpu.make_async_copy(ref, ref, sem).wait()


def kernel(
    w_in, new_in, mom_in, x_in, inc_in, g_in, loss_in, kept_in,
    f_out, b_out, w_out, m_out,
    w, x, kept, part, part_in, half, half_in, grad, f_own, b_own, f_send, b_send,
    inc, loss, scaled, p1, p1_in, p2, p2_in, kw, ks, keep0, dw, dw_in, own_sum, kept_pair, scaled_pair, new, mom, w_new, m_new,
    load, fz_r, fz_s, fx_r, fx_s, kz_r, kz_s, kx_r, kx_s, rx_r, rx_s, rz_r, rz_s,
    p1_r, p1_s, p2_r, p2_s, g_r, g_s, pk_r, pk_s, ps_r, ps_s, dp_r, dp_s, out_sem,
):
    blocks, depth, own_cols = w.shape
    ticks, rows = x.shape[0], x.shape[2]
    extent = blocks * depth
    inv_root = 1.0 / float(extent) ** 0.5
    s, r, j = lax.axis_index("section"), lax.axis_index("dp"), lax.axis_index("tensor")
    sections, replicas = lax.axis_size("section"), lax.axis_size("dp")
    col, rank = lax.div(j, SIDE), lax.rem(j, SIDE)
    up, down = lax.rem(s + 1, sections), lax.rem(s + sections - 1, sections)
    is_first, is_last = s == 0, s == sections - 1
    pair = r + 1 - 2 * lax.rem(r, 2)
    far = lax.rem(r + 2, replicas)
    beyond = lax.rem(pair + 2, replicas)

    def xs(e):
        return lax.rem(col + e + SIDE, SIDE)

    def zs(d):
        return lax.rem(rank + d + SIDE, SIDE)

    def remote(src, dst, send, recv, device):
        pltpu.make_async_remote_copy(
            src_ref=src, dst_ref=dst, send_sem=send, recv_sem=recv,
            device_id=device, device_id_type=MESH,
        ).start()

    barrier = pltpu.get_barrier_semaphore()
    peers = [(s, r, xs(e) * SIDE + rank) for e in range(1, SIDE)]
    peers += [(s, r, col * SIDE + zs(d)) for d in range(1, SIDE)]
    peers += [(q, r, col * SIDE + zs(d)) for q in (up, down) for d in range(SIDE)]
    peers += [(s, lax.rem(r + f, replicas), j) for f in range(1, replicas)]
    for peer in peers:
        pl.semaphore_signal(barrier, inc=1, device_id=peer, device_id_type=MESH)

    loads = [
        pltpu.make_async_copy(src, dst, load.at[i])
        for i, (src, dst) in enumerate([
            (x_in, x.at[0, j]), (g_in, grad.at[0]), (kept_in, kept.at[j]), (w_in, w),
            (inc_in, inc), (loss_in, loss), (new_in, new), (mom_in, mom),
        ])
    ]
    for copy in loads:
        copy.start()
    for copy in loads[:3]:
        copy.wait()
    pl.semaphore_wait(barrier, len(peers))

    def kept_to_z(t):
        mine = kept.at[j, pl.ds(pl.multiple_of(t * rows, rows), rows), :]
        for d in NEAR_LAST[:3]:
            remote(mine, mine, kz_s.at[t], kz_r.at[t], (s, r, col * SIDE + zs(d)))

    def kept_to_x(t):
        span = pl.ds(pl.multiple_of(t * rows, rows), rows)
        local_wait(kept.at[pl.ds(0, SIDE - 1), span, :], kz_r.at[t])
        group = kept.at[pl.ds(col * SIDE, SIDE), span, :]
        for e in NEAR_LAST[:3]:
            remote(group, group, kx_s.at[t], kx_r.at[t], (s, r, xs(e) * SIDE + rank))

    kept_to_z(0)
    for d in NEAR_LAST[:3]:
        remote(x.at[0, j], x.at[0, j], fz_s.at[0], fz_r.at[0, d], (s, r, col * SIDE + zs(d)))

    loads[3].wait()
    loads[4].wait()
    loads[5].wait()

    row_id = lax.broadcasted_iota(jnp.int32, (rows, 128), 0)
    lane_id = lax.broadcasted_iota(jnp.int32, (rows, 128), 1)
    diagonal = row_id == lane_id

    def kept_to_pair(t):
        span = pl.ds(pl.multiple_of(t * rows, rows), rows)
        for i, owner in ((1, beyond), (0, pair)):
            remote(
                kept.at[pl.ds(owner * SIDE, SIDE), span, :], kept_pair.at[i, :, span, :],
                pk_s.at[t], pk_r.at[t], (s, pair, j),
            )

    def kept_products(t):
        span = pl.ds(pl.multiple_of(t * rows, rows), rows)
        local_wait(kept.at[pl.ds(0, SIDE * (SIDE - 1)), span, :], kx_r.at[t])
        product = jnp.zeros((rows, own_cols), F32)
        squares = jnp.zeros((rows, own_cols), F32)
        for k in range(blocks):
            block = kept[k, span, :]
            product += jnp.dot(block, w[k], preferred_element_type=F32)
            wide = block.astype(F32)
            squares += wide * wide
        found = lax.rsqrt(jnp.sum(squares, axis=-1, keepdims=True) / extent + EPSILON)
        kw[...] = product * (found * inv_root)
        ks[...] = jnp.broadcast_to(found, (rows, 128))

    def row_products(t):
        span = pl.ds(pl.multiple_of(t * rows, rows), rows)
        g_wide = grad[t].astype(F32)
        scaled[span, :] = (g_wide * ks[:, :1]).astype(BF16)
        remote(
            scaled.at[span, :], scaled_pair.at[span, :], ps_s.at[t], ps_r.at[t], (s, pair, j)
        )
        dots = jnp.sum(g_wide * kw[...], axis=-1, keepdims=True)
        p1[t] = jnp.sum(jnp.where(diagonal, dots, 0.0), axis=0, keepdims=True)
        for e in NEAR_LAST[:3]:
            remote(
                p1.at[t], p1_in.at[t, e - 1], p1_s.at[t], p1_r.at[t],
                (s, r, xs(e) * SIDE + rank),
            )

    def row_products_over_x(t):
        local_wait(p1_in.at[t], p1_r.at[t])
        p2[t] = p1[t] + p1_in[t, 0] + p1_in[t, 1] + p1_in[t, 2]
        for d in NEAR_LAST[:3]:
            remote(
                p2.at[t], p2_in.at[t, d - 1], p2_s.at[t], p2_r.at[t],
                (s, r, col * SIDE + zs(d)),
            )

    def pair_gradient(owner, i, c):
        over_rows = (((0,), (0,)), ((), ()))
        term = lax.dot_general(
            kept[owner * SIDE + c], scaled[...], over_rows, preferred_element_type=F32
        )
        term += lax.dot_general(
            kept_pair[i, c], scaled_pair[...], over_rows, preferred_element_type=F32
        )
        return term * inv_root

    def tick(t, carry):
        span = pl.ds(pl.multiple_of(t * rows, rows), rows)

        @pl.when(t > 0)
        def _():
            kept_products(t)

            @pl.when(t == ticks - 1)
            def _():
                kept_to_pair(t)

            local_wait(grad.at[0], g_r.at[t])
            row_products(t)

        g = grad[t]
        for d in NEAR_LAST:
            for e in NEAR_LAST:
                k = xs(e) * SIDE + zs(d)
                term = lax.dot_general(
                    g, w[k], (((1,), (1,)), ((), ())), preferred_element_type=F32
                )
                part[t, k] = (term * inv_root).astype(BF16)
                if e:
                    remote(
                        part.at[t, k], part_in.at[t, d, e - 1], rx_s.at[t], rx_r.at[t, d],
                        (s, r, xs(e) * SIDE + rank),
                    )

        def pass_on(d):
            k = col * SIDE + zs(-d)
            for e in NEAR_LAST[:3]:
                remote(
                    x.at[t, k], x.at[t, k], fx_s.at[t], fx_r.at[t, d],
                    (s, r, xs(e) * SIDE + rank),
                )

        @pl.when(t > 0)
        def _():
            local_wait(x.at[t, 0], fz_r.at[t, 0])

        pass_on(0)

        def over_x(d):
            local_wait(part_in.at[t, d], rx_r.at[t, d])
            total = part[t, col * SIDE + zs(d)].astype(F32)
            for e in range(SIDE - 1):
                total += part_in[t, d, e].astype(F32)
            return total

        for d in (2, 1, 3):
            half[t, d - 1] = over_x(d).astype(BF16)
            remote(
                half.at[t, d - 1], half_in.at[t, d - 1], rz_s.at[t], rz_r.at[t],
                (s, r, col * SIDE + zs(d)),
            )
            if d != 2:
                local_wait(x.at[t, 0], fz_r.at[t, d])
                pass_on(d)
        keep0[...] = over_x(0)

        @pl.when(t == 0)
        def _():
            kept_to_x(0)
            kept_to_z(1)

        local_wait(x.at[t, 0], fz_r.at[t, 2])
        pass_on(2)

        @pl.when(t == 0)
        def _():
            kept_products(0)
            row_products(0)

        @pl.when(t > 0)
        def _():
            row_products_over_x(t)

        @pl.when((t > 0) & (t < ticks - 1))
        def _():
            kept_to_x(t + 1)


        @pl.when(t == ticks - 1)
        def _():
            for u in range(ticks):
                rows_u = pl.ds(u * rows, rows)
                local_wait(kept_pair.at[:, :, rows_u, :], pk_r.at[u])
                local_wait(scaled_pair.at[rows_u, :], ps_r.at[u])
            for c in range(SIDE):
                dw[c] = pair_gradient(far, 1, c).astype(BF16)
                remote(dw.at[c], dw_in.at[c], dp_s, dp_r.at[c], (s, far, j))

        total = jnp.zeros((rows, own_cols), F32)
        squares = jnp.zeros((rows, own_cols), F32)
        for d in NEAR_FIRST:
            local_wait(x.at[t, pl.ds(0, SIDE - 1)], fx_r.at[t, d])
            for e in range(SIDE):
                k = xs(-e) * SIDE + zs(-d)
                block = x[t, k]
                total += jnp.dot(block, w[k], preferred_element_type=F32)
                wide = block.astype(F32)
                squares += wide * wide
        scale = lax.rsqrt(jnp.sum(squares, axis=-1, keepdims=True) / extent + EPSILON)
        result = (x[t, j].astype(F32) + total * scale * inv_root).astype(BF16)
        f_own[t] = result

        @pl.when(t < ticks - 1)
        def _():
            f_send[t] = jnp.where(is_last, inc[jnp.minimum(t, ticks - 2)], result)
            for d in NEAR_LAST:
                remote(
                    f_send.at[t], x.at[t + 1, j], fz_s.at[t + 1], fz_r.at[t + 1, d],
                    (up, r, col * SIDE + zs(d)),
                )

        @pl.when((t > 0) & (t < ticks - 2))
        def _():
            kept_to_z(t + 2)

        @pl.when((t > 0) & (t < ticks - 1))
        def _():
            kept_to_pair(t)

        @pl.when(t == 0)
        def _():
            row_products_over_x(t)
            kept_to_x(1)
            kept_to_z(2)
            kept_to_pair(0)

        local_wait(half_in.at[t], rz_r.at[t])
        branch = keep0[...]
        for d in range(SIDE - 1):
            branch += half_in[t, d].astype(F32)
        local_wait(p2_in.at[t], p2_r.at[t])
        line = p2[t] + p2_in[t, 0] + p2_in[t, 1] + p2_in[t, 2]
        inner = jnp.sum(jnp.where(diagonal, line, 0.0), axis=-1, keepdims=True) / extent
        kept_scale = ks[:, :1]
        hat = kept[j, span, :].astype(F32) * kept_scale
        back = (grad[t].astype(F32) + (branch - hat * inner) * kept_scale).astype(BF16)
        b_own[t] = back

        @pl.when(t < ticks - 1)
        def _():
            b_send[t] = jnp.where(is_first, loss[jnp.minimum(t, ticks - 2)], back)
            remote(b_send.at[t], grad.at[t + 1], g_s.at[t + 1], g_r.at[t + 1], (down, r, j))

        return carry

    lax.fori_loop(0, ticks, tick, 0)

    outs = [
        pltpu.make_async_copy(f_own, f_out, out_sem.at[0]),
        pltpu.make_async_copy(b_own, b_out, out_sem.at[1]),
    ]
    for copy in outs:
        copy.start()
    loads[6].wait()
    loads[7].wait()
    for c in range(SIDE):
        own_sum[c] = pair_gradient(r, 0, c)
    for c in range(SIDE):
        local_wait(dw_in.at[c], dp_r.at[c])
        velocity = MOMENTUM_RATE * mom[c].astype(F32) + (own_sum[c] + dw_in[c].astype(F32))
        w_new[c] = (new[c].astype(F32) - LEARNING_RATE * velocity).astype(BF16)
        m_new[c] = velocity.astype(BF16)
        more = [
            pltpu.make_async_copy(w_new.at[c], w_out.at[c], out_sem.at[2 + 2 * c]),
            pltpu.make_async_copy(m_new.at[c], m_out.at[c], out_sem.at[3 + 2 * c]),
        ]
        for copy in more:
            copy.start()
        outs += more

    for t in range(ticks):
        local_wait(x.at[0, pl.ds(0, SIDE if t else SIDE - 1)], fz_s.at[t])
        local_wait(x.at[0, pl.ds(0, SIDE * (SIDE - 1))], fx_s.at[t])
        local_wait(x.at[0, pl.ds(0, SIDE - 1)], kz_s.at[t])
        local_wait(x.at[0, pl.ds(0, SIDE * (SIDE - 1))], kx_s.at[t])
        local_wait(x.at[0, pl.ds(0, SIDE * (SIDE - 1))], rx_s.at[t])
        local_wait(x.at[0, pl.ds(0, SIDE - 1)], rz_s.at[t])
        local_wait(p1_in.at[0], p1_s.at[t])
        local_wait(p2_in.at[0], p2_s.at[t])
        local_wait(x.at[0, pl.ds(0, 2 * SIDE)], pk_s.at[t])
        local_wait(grad.at[0], ps_s.at[t])
        if t:
            local_wait(grad.at[0], g_s.at[t])
    local_wait(dw, dp_s)
    for copy in outs:
        copy.wait()


def hand_over(f_in, b_in, w_in, m_in, f_out, b_out, w_out, m_out, f, b, w, m, sem):
    pairs = [(f_in, f, f_out), (b_in, b, b_out), (w_in, w, w_out), (m_in, m, m_out)]
    reads = [pltpu.make_async_copy(a, v, sem.at[0, i]) for i, (a, v, _) in enumerate(pairs)]
    writes = [pltpu.make_async_copy(v, o, sem.at[1, i]) for i, (_, v, o) in enumerate(pairs)]
    for copy in reads:
        copy.start()
    for read, write in zip(reads, writes):
        read.wait()
        write.start()
    for copy in writes:
        copy.wait()


def body(
    shadow_weight_copy, newest_weight_version, momentum, pending_section_input,
    incoming_micro_input, pending_output_gradient, loss_gradient_rows, stashed,
):
    extent, cols = shadow_weight_copy.shape[1:]
    ticks, rows = stashed.shape[2:4]
    part_rows = newest_weight_version.shape[1]
    replicas = extent // part_rows
    blocks = extent // cols
    chunk = part_rows // SIDE

    vmem, dma = pltpu.VMEM, pltpu.SemaphoreType.DMA
    block = (rows, cols)
    scratch = [
        vmem((blocks, cols, cols), BF16),
        vmem((ticks, blocks, *block), BF16),
        vmem((blocks, ticks * rows, cols), BF16),
        vmem((ticks, blocks, *block), BF16),
        vmem((ticks, SIDE, SIDE - 1, *block), BF16),
        vmem((ticks, SIDE - 1, *block), BF16),
        vmem((ticks, SIDE - 1, *block), BF16),
        vmem((ticks, *block), BF16),
        vmem((ticks, *block), BF16),
        vmem((ticks, *block), BF16),
        vmem((ticks - 1, *block), BF16),
        vmem((ticks - 1, *block), BF16),
        vmem((ticks - 1, *block), BF16),
        vmem((ticks - 1, *block), BF16),
        vmem((ticks * rows, cols), BF16),
        vmem((ticks, 1, 128), F32),
        vmem((ticks, SIDE - 1, 1, 128), F32),
        vmem((ticks, 1, 128), F32),
        vmem((ticks, SIDE - 1, 1, 128), F32),
        vmem(block, F32),
        vmem((rows, 128), F32),
        vmem(block, F32),
        vmem((SIDE, chunk, cols), BF16),
        vmem((SIDE, chunk, cols), BF16),
        vmem((SIDE, chunk, cols), F32),
        vmem((2, SIDE, ticks * rows, cols), BF16),
        vmem((ticks * rows, cols), BF16),
        vmem((SIDE, chunk, cols), BF16),
        vmem((SIDE, chunk, cols), BF16),
        vmem((SIDE, chunk, cols), BF16),
        vmem((SIDE, chunk, cols), BF16),
        dma((8,)),
        dma((ticks, SIDE)), dma((ticks,)),
        dma((ticks, SIDE)), dma((ticks,)),
        dma((ticks,)), dma((ticks,)),
        dma((ticks,)), dma((ticks,)),
        dma((ticks, SIDE)), dma((ticks,)),
        dma((ticks,)), dma((ticks,)),
        dma((ticks,)), dma((ticks,)),
        dma((ticks,)), dma((ticks,)),
        dma((ticks,)), dma((ticks,)),
        dma((ticks,)), dma((ticks,)),
        dma((ticks,)), dma((ticks,)),
        dma((SIDE,)), dma,
        dma((2 + 2 * SIDE,)),
    ]
    any_space = pl.BlockSpec(memory_space=pl.ANY)
    shape = jax.ShapeDtypeStruct
    f_out, b_out, w_out, m_out = pl.pallas_call(
        kernel,
        name="window",
        out_shape=(
            shape((ticks, *block), BF16),
            shape((ticks, *block), BF16),
            shape((SIDE, chunk, cols), BF16),
            shape((SIDE, chunk, cols), BF16),
        ),
        in_specs=[any_space] * 8,
        out_specs=(any_space,) * 4,
        scratch_shapes=scratch,
        compiler_params=pltpu.CompilerParams(
            collective_id=0, has_side_effects=True, vmem_limit_bytes=60 * 1024 * 1024
        ),
    )(
        shadow_weight_copy.reshape(blocks, cols, cols),
        newest_weight_version.reshape(SIDE, chunk, cols),
        momentum.reshape(SIDE, chunk, cols),
        pending_section_input.reshape(block),
        incoming_micro_input.reshape(ticks - 1, *block),
        pending_output_gradient.reshape(block),
        loss_gradient_rows.reshape(ticks - 1, *block),
        stashed.reshape(ticks * rows, cols),
    )
    f_out, b_out, w_out, m_out = pl.pallas_call(
        hand_over,
        name="hand_over",
        out_shape=(
            shape((ticks, *block), BF16),
            shape((ticks, *block), BF16),
            shape((SIDE, chunk, cols), BF16),
            shape((SIDE, chunk, cols), BF16),
        ),
        in_specs=[any_space] * 4,
        out_specs=(any_space,) * 4,
        scratch_shapes=[
            vmem((ticks, *block), BF16),
            vmem((ticks, *block), BF16),
            vmem((SIDE, chunk, cols), BF16),
            vmem((SIDE, chunk, cols), BF16),
            dma((2, 4)),
        ],
    )(f_out, b_out, w_out, m_out)
    return (
        f_out[None, None],
        b_out[None, None],
        w_out.reshape(1, part_rows, cols),
        m_out.reshape(1, part_rows, cols),
    )


def solution(mesh):
    return jax.shard_map(
        body,
        mesh=mesh,
        in_specs=(
            P("section", None, "tensor"),
            P("section", "dp", "tensor"),
            P("section", "dp", "tensor"),
            P("dp", "section", None, "tensor"),
            P("dp", None, None, "tensor"),
            P("dp", "section", None, "tensor"),
            P("dp", None, None, "tensor"),
            P("dp", "section", None, None, "tensor"),
        ),
        out_specs=(
            P("dp", "section", None, None, "tensor"),
            P("dp", "section", None, None, "tensor"),
            P("section", "dp", "tensor"),
            P("section", "dp", "tensor"),
        ),
        check_vma=False,
    )
```

```python
import functools

import jax
import jax.numpy as jnp
from jax import lax
from jax.experimental import pallas as pl
from jax.experimental.pallas import tpu as pltpu
from jax.sharding import PartitionSpec as P

EPSILON = 1e-06
MOMENTUM_RATE = 0.9
LEARNING_RATE = 0.05
MESH = pl.DeviceIdType.MESH
F32 = jnp.float32
BF16 = jnp.bfloat16

SIDE = 4
NEAR_LAST = (2, 1, 3, 0)
NEAR_FIRST = (0, 1, 3, 2)


def local_wait(ref, sem):
    pltpu.make_async_copy(ref, ref, sem).wait()


def kernel(
    w_in, new_in, mom_in, x_in, inc_in, g_in, loss_in, kept_in,
    f_out, b_out, w_out, m_out,
    w, x, kept, part, part_in, half, half_in, grad, f_own, b_own, f_send, b_send,
    inc, loss, scaled, p1, p1_in, p2, p2_in, kw, ks, keep0, dw, dw_in, own_sum, kept_pair, scaled_pair, new, mom, w_new, m_new,
    load, fz_r, fz_s, fx_r, fx_s, kz_r, kz_s, kx_r, kx_s, rx_r, rx_s, rz_r, rz_s,
    p1_r, p1_s, p2_r, p2_s, g_r, g_s, pk_r, pk_s, ps_r, ps_s, dp_r, dp_s, out_sem,
):
    blocks, depth, own_cols = w.shape
    ticks, rows = x.shape[0], x.shape[2]
    extent = blocks * depth
    inv_root = 1.0 / float(extent) ** 0.5
    s, r, j = lax.axis_index("section"), lax.axis_index("dp"), lax.axis_index("tensor")
    sections, replicas = lax.axis_size("section"), lax.axis_size("dp")
    col, rank = lax.div(j, SIDE), lax.rem(j, SIDE)
    up, down = lax.rem(s + 1, sections), lax.rem(s + sections - 1, sections)
    is_first, is_last = s == 0, s == sections - 1
    pair = r + 1 - 2 * lax.rem(r, 2)
    far = lax.rem(r + 2, replicas)
    beyond = lax.rem(pair + 2, replicas)

    def xs(e):
        return lax.rem(col + e + SIDE, SIDE)

    def zs(d):
        return lax.rem(rank + d + SIDE, SIDE)

    def remote(src, dst, send, recv, device):
        pltpu.make_async_remote_copy(
            src_ref=src, dst_ref=dst, send_sem=send, recv_sem=recv,
            device_id=device, device_id_type=MESH,
        ).start()

    barrier = pltpu.get_barrier_semaphore()
    peers = [(s, r, xs(e) * SIDE + rank) for e in range(1, SIDE)]
    peers += [(s, r, col * SIDE + zs(d)) for d in range(1, SIDE)]
    peers += [(q, r, col * SIDE + zs(d)) for q in (up, down) for d in range(SIDE)]
    peers += [(s, lax.rem(r + f, replicas), j) for f in range(1, replicas)]
    for peer in peers:
        pl.semaphore_signal(barrier, inc=1, device_id=peer, device_id_type=MESH)

    loads = [
        pltpu.make_async_copy(src, dst, load.at[i])
        for i, (src, dst) in enumerate([
            (x_in, x.at[0, j]), (g_in, grad.at[0]), (kept_in, kept.at[j]), (w_in, w),
            (inc_in, inc), (loss_in, loss), (new_in, new), (mom_in, mom),
        ])
    ]
    for copy in loads:
        copy.start()
    for copy in loads[:3]:
        copy.wait()
    pl.semaphore_wait(barrier, len(peers))

    def kept_to_z(t):
        mine = kept.at[j, pl.ds(pl.multiple_of(t * rows, rows), rows), :]
        for d in NEAR_LAST[:3]:
            remote(mine, mine, kz_s.at[t], kz_r.at[t], (s, r, col * SIDE + zs(d)))

    def kept_to_x(t):
        span = pl.ds(pl.multiple_of(t * rows, rows), rows)
        local_wait(kept.at[pl.ds(0, SIDE - 1), span, :], kz_r.at[t])
        group = kept.at[pl.ds(col * SIDE, SIDE), span, :]
        for e in NEAR_LAST[:3]:
            remote(group, group, kx_s.at[t], kx_r.at[t], (s, r, xs(e) * SIDE + rank))

    kept_to_z(0)
    for d in NEAR_LAST[:3]:
        remote(x.at[0, j], x.at[0, j], fz_s.at[0], fz_r.at[0, d], (s, r, col * SIDE + zs(d)))

    loads[3].wait()
    loads[4].wait()
    loads[5].wait()

    row_id = lax.broadcasted_iota(jnp.int32, (rows, 128), 0)
    lane_id = lax.broadcasted_iota(jnp.int32, (rows, 128), 1)
    diagonal = row_id == lane_id

    def kept_to_pair(t):
        span = pl.ds(pl.multiple_of(t * rows, rows), rows)
        for i, owner in ((1, beyond), (0, pair)):
            remote(
                kept.at[pl.ds(owner * SIDE, SIDE), span, :], kept_pair.at[i, :, span, :],
                pk_s.at[t], pk_r.at[t], (s, pair, j),
            )

    def kept_products(t):
        span = pl.ds(pl.multiple_of(t * rows, rows), rows)
        local_wait(kept.at[pl.ds(0, SIDE * (SIDE - 1)), span, :], kx_r.at[t])
        product = jnp.zeros((rows, own_cols), F32)
        squares = jnp.zeros((rows, own_cols), F32)
        for k in range(blocks):
            block = kept[k, span, :]
            product += jnp.dot(block, w[k], preferred_element_type=F32)
            wide = block.astype(F32)
            squares += wide * wide
        found = lax.rsqrt(jnp.sum(squares, axis=-1, keepdims=True) / extent + EPSILON)
        kw[...] = product * (found * inv_root)
        ks[...] = jnp.broadcast_to(found, (rows, 128))

    def row_products(t):
        span = pl.ds(pl.multiple_of(t * rows, rows), rows)
        g_wide = grad[t].astype(F32)
        scaled[span, :] = (g_wide * ks[:, :1]).astype(BF16)
        remote(
            scaled.at[span, :], scaled_pair.at[span, :], ps_s.at[t], ps_r.at[t], (s, pair, j)
        )
        dots = jnp.sum(g_wide * kw[...], axis=-1, keepdims=True)
        p1[t] = jnp.sum(jnp.where(diagonal, dots, 0.0), axis=0, keepdims=True)
        for e in NEAR_LAST[:3]:
            remote(
                p1.at[t], p1_in.at[t, e - 1], p1_s.at[t], p1_r.at[t],
                (s, r, xs(e) * SIDE + rank),
            )

    def row_products_over_x(t):
        local_wait(p1_in.at[t], p1_r.at[t])
        p2[t] = p1[t] + p1_in[t, 0] + p1_in[t, 1] + p1_in[t, 2]
        for d in NEAR_LAST[:3]:
            remote(
                p2.at[t], p2_in.at[t, d - 1], p2_s.at[t], p2_r.at[t],
                (s, r, col * SIDE + zs(d)),
            )

    def pair_gradient(owner, i, c):
        over_rows = (((0,), (0,)), ((), ()))
        term = lax.dot_general(
            kept[owner * SIDE + c], scaled[...], over_rows, preferred_element_type=F32
        )
        term += lax.dot_general(
            kept_pair[i, c], scaled_pair[...], over_rows, preferred_element_type=F32
        )
        return term * inv_root

    def tick(t, carry):
        span = pl.ds(pl.multiple_of(t * rows, rows), rows)

        @pl.when(t > 0)
        def _():
            kept_products(t)

            @pl.when(t == ticks - 1)
            def _():
                kept_to_pair(t)

            local_wait(grad.at[0], g_r.at[t])
            row_products(t)

        g = grad[t]
        for d in NEAR_LAST:
            for e in NEAR_LAST:
                k = xs(e) * SIDE + zs(d)
                term = lax.dot_general(
                    g, w[k], (((1,), (1,)), ((), ())), preferred_element_type=F32
                )
                part[t, k] = (term * inv_root).astype(BF16)
                if e:
                    remote(
                        part.at[t, k], part_in.at[t, d, e - 1], rx_s.at[t], rx_r.at[t, d],
                        (s, r, xs(e) * SIDE + rank),
                    )

        def pass_on(d):
            k = col * SIDE + zs(-d)
            for e in NEAR_LAST[:3]:
                remote(
                    x.at[t, k], x.at[t, k], fx_s.at[t], fx_r.at[t, d],
                    (s, r, xs(e) * SIDE + rank),
                )

        @pl.when(t > 0)
        def _():
            local_wait(x.at[t, 0], fz_r.at[t, 0])

        pass_on(0)

        def over_x(d):
            local_wait(part_in.at[t, d], rx_r.at[t, d])
            total = part[t, col * SIDE + zs(d)].astype(F32)
            for e in range(SIDE - 1):
                total += part_in[t, d, e].astype(F32)
            return total

        for d in (2, 1, 3):
            half[t, d - 1] = over_x(d).astype(BF16)
            remote(
                half.at[t, d - 1], half_in.at[t, d - 1], rz_s.at[t], rz_r.at[t],
                (s, r, col * SIDE + zs(d)),
            )
            if d != 2:
                local_wait(x.at[t, 0], fz_r.at[t, d])
                pass_on(d)
        keep0[...] = over_x(0)

        local_wait(x.at[t, 0], fz_r.at[t, 2])
        pass_on(2)

        @pl.when(t == 0)
        def _():
            kept_to_x(0)
            kept_to_z(1)

        @pl.when(t > 0)
        def _():
            row_products_over_x(t)

        @pl.when((t > 0) & (t < ticks - 1))
        def _():
            kept_to_x(t + 1)


        @pl.when(t == ticks - 1)
        def _():
            for u in range(ticks):
                rows_u = pl.ds(u * rows, rows)
                local_wait(kept_pair.at[:, :, rows_u, :], pk_r.at[u])
                local_wait(scaled_pair.at[rows_u, :], ps_r.at[u])
            for c in range(SIDE):
                dw[c] = pair_gradient(far, 1, c).astype(BF16)
                remote(dw.at[c], dw_in.at[c], dp_s, dp_r.at[c], (s, far, j))

        total = jnp.zeros((rows, own_cols), F32)
        squares = jnp.zeros((rows, own_cols), F32)
        for d in NEAR_FIRST:
            local_wait(x.at[t, pl.ds(0, SIDE - 1)], fx_r.at[t, d])
            for e in range(SIDE):
                k = xs(-e) * SIDE + zs(-d)
                block = x[t, k]
                total += jnp.dot(block, w[k], preferred_element_type=F32)
                wide = block.astype(F32)
                squares += wide * wide
        scale = lax.rsqrt(jnp.sum(squares, axis=-1, keepdims=True) / extent + EPSILON)
        result = (x[t, j].astype(F32) + total * scale * inv_root).astype(BF16)
        f_own[t] = result

        @pl.when(t < ticks - 1)
        def _():
            f_send[t] = jnp.where(is_last, inc[jnp.minimum(t, ticks - 2)], result)
            for d in NEAR_LAST:
                remote(
                    f_send.at[t], x.at[t + 1, j], fz_s.at[t + 1], fz_r.at[t + 1, d],
                    (up, r, col * SIDE + zs(d)),
                )

        @pl.when((t > 0) & (t < ticks - 2))
        def _():
            kept_to_z(t + 2)

        @pl.when((t > 0) & (t < ticks - 1))
        def _():
            kept_to_pair(t)

        @pl.when(t == 0)
        def _():
            kept_products(0)
            row_products(0)
            kept_to_x(1)
            row_products_over_x(0)
            kept_to_z(2)
            kept_to_pair(0)

        local_wait(half_in.at[t], rz_r.at[t])
        branch = keep0[...]
        for d in range(SIDE - 1):
            branch += half_in[t, d].astype(F32)
        local_wait(p2_in.at[t], p2_r.at[t])
        line = p2[t] + p2_in[t, 0] + p2_in[t, 1] + p2_in[t, 2]
        inner = jnp.sum(jnp.where(diagonal, line, 0.0), axis=-1, keepdims=True) / extent
        kept_scale = ks[:, :1]
        hat = kept[j, span, :].astype(F32) * kept_scale
        back = (grad[t].astype(F32) + (branch - hat * inner) * kept_scale).astype(BF16)
        b_own[t] = back

        @pl.when(t < ticks - 1)
        def _():
            b_send[t] = jnp.where(is_first, loss[jnp.minimum(t, ticks - 2)], back)
            remote(b_send.at[t], grad.at[t + 1], g_s.at[t + 1], g_r.at[t + 1], (down, r, j))

        return carry

    lax.fori_loop(0, ticks, tick, 0)

    outs = [
        pltpu.make_async_copy(f_own, f_out, out_sem.at[0]),
        pltpu.make_async_copy(b_own, b_out, out_sem.at[1]),
    ]
    for copy in outs:
        copy.start()
    loads[6].wait()
    loads[7].wait()
    for c in range(SIDE):
        own_sum[c] = pair_gradient(r, 0, c)
    for c in range(SIDE):
        local_wait(dw_in.at[c], dp_r.at[c])
        velocity = MOMENTUM_RATE * mom[c].astype(F32) + (own_sum[c] + dw_in[c].astype(F32))
        w_new[c] = (new[c].astype(F32) - LEARNING_RATE * velocity).astype(BF16)
        m_new[c] = velocity.astype(BF16)
        more = [
            pltpu.make_async_copy(w_new.at[c], w_out.at[c], out_sem.at[2 + 2 * c]),
            pltpu.make_async_copy(m_new.at[c], m_out.at[c], out_sem.at[3 + 2 * c]),
        ]
        for copy in more:
            copy.start()
        outs += more

    for t in range(ticks):
        local_wait(x.at[0, pl.ds(0, SIDE if t else SIDE - 1)], fz_s.at[t])
        local_wait(x.at[0, pl.ds(0, SIDE * (SIDE - 1))], fx_s.at[t])
        local_wait(x.at[0, pl.ds(0, SIDE - 1)], kz_s.at[t])
        local_wait(x.at[0, pl.ds(0, SIDE * (SIDE - 1))], kx_s.at[t])
        local_wait(x.at[0, pl.ds(0, SIDE * (SIDE - 1))], rx_s.at[t])
        local_wait(x.at[0, pl.ds(0, SIDE - 1)], rz_s.at[t])
        local_wait(p1_in.at[0], p1_s.at[t])
        local_wait(p2_in.at[0], p2_s.at[t])
        local_wait(x.at[0, pl.ds(0, 2 * SIDE)], pk_s.at[t])
        local_wait(grad.at[0], ps_s.at[t])
        if t:
            local_wait(grad.at[0], g_s.at[t])
    local_wait(dw, dp_s)
    for copy in outs:
        copy.wait()


def hand_over(f_in, b_in, w_in, m_in, f_out, b_out, w_out, m_out, f, b, w, m, sem):
    pairs = [(f_in, f, f_out), (b_in, b, b_out), (w_in, w, w_out), (m_in, m, m_out)]
    reads = [pltpu.make_async_copy(a, v, sem.at[0, i]) for i, (a, v, _) in enumerate(pairs)]
    writes = [pltpu.make_async_copy(v, o, sem.at[1, i]) for i, (_, v, o) in enumerate(pairs)]
    for copy in reads:
        copy.start()
    for read, write in zip(reads, writes):
        read.wait()
        write.start()
    for copy in writes:
        copy.wait()


def body(
    shadow_weight_copy, newest_weight_version, momentum, pending_section_input,
    incoming_micro_input, pending_output_gradient, loss_gradient_rows, stashed,
):
    extent, cols = shadow_weight_copy.shape[1:]
    ticks, rows = stashed.shape[2:4]
    part_rows = newest_weight_version.shape[1]
    replicas = extent // part_rows
    blocks = extent // cols
    chunk = part_rows // SIDE

    vmem, dma = pltpu.VMEM, pltpu.SemaphoreType.DMA
    block = (rows, cols)
    scratch = [
        vmem((blocks, cols, cols), BF16),
        vmem((ticks, blocks, *block), BF16),
        vmem((blocks, ticks * rows, cols), BF16),
        vmem((ticks, blocks, *block), BF16),
        vmem((ticks, SIDE, SIDE - 1, *block), BF16),
        vmem((ticks, SIDE - 1, *block), BF16),
        vmem((ticks, SIDE - 1, *block), BF16),
        vmem((ticks, *block), BF16),
        vmem((ticks, *block), BF16),
        vmem((ticks, *block), BF16),
        vmem((ticks - 1, *block), BF16),
        vmem((ticks - 1, *block), BF16),
        vmem((ticks - 1, *block), BF16),
        vmem((ticks - 1, *block), BF16),
        vmem((ticks * rows, cols), BF16),
        vmem((ticks, 1, 128), F32),
        vmem((ticks, SIDE - 1, 1, 128), F32),
        vmem((ticks, 1, 128), F32),
        vmem((ticks, SIDE - 1, 1, 128), F32),
        vmem(block, F32),
        vmem((rows, 128), F32),
        vmem(block, F32),
        vmem((SIDE, chunk, cols), BF16),
        vmem((SIDE, chunk, cols), BF16),
        vmem((SIDE, chunk, cols), F32),
        vmem((2, SIDE, ticks * rows, cols), BF16),
        vmem((ticks * rows, cols), BF16),
        vmem((SIDE, chunk, cols), BF16),
        vmem((SIDE, chunk, cols), BF16),
        vmem((SIDE, chunk, cols), BF16),
        vmem((SIDE, chunk, cols), BF16),
        dma((8,)),
        dma((ticks, SIDE)), dma((ticks,)),
        dma((ticks, SIDE)), dma((ticks,)),
        dma((ticks,)), dma((ticks,)),
        dma((ticks,)), dma((ticks,)),
        dma((ticks, SIDE)), dma((ticks,)),
        dma((ticks,)), dma((ticks,)),
        dma((ticks,)), dma((ticks,)),
        dma((ticks,)), dma((ticks,)),
        dma((ticks,)), dma((ticks,)),
        dma((ticks,)), dma((ticks,)),
        dma((ticks,)), dma((ticks,)),
        dma((SIDE,)), dma,
        dma((2 + 2 * SIDE,)),
    ]
    any_space = pl.BlockSpec(memory_space=pl.ANY)
    shape = jax.ShapeDtypeStruct
    f_out, b_out, w_out, m_out = pl.pallas_call(
        kernel,
        name="window",
        out_shape=(
            shape((ticks, *block), BF16),
            shape((ticks, *block), BF16),
            shape((SIDE, chunk, cols), BF16),
            shape((SIDE, chunk, cols), BF16),
        ),
        in_specs=[any_space] * 8,
        out_specs=(any_space,) * 4,
        scratch_shapes=scratch,
        compiler_params=pltpu.CompilerParams(
            collective_id=0, has_side_effects=True, vmem_limit_bytes=60 * 1024 * 1024
        ),
    )(
        shadow_weight_copy.reshape(blocks, cols, cols),
        newest_weight_version.reshape(SIDE, chunk, cols),
        momentum.reshape(SIDE, chunk, cols),
        pending_section_input.reshape(block),
        incoming_micro_input.reshape(ticks - 1, *block),
        pending_output_gradient.reshape(block),
        loss_gradient_rows.reshape(ticks - 1, *block),
        stashed.reshape(ticks * rows, cols),
    )
    f_out, b_out, w_out, m_out = pl.pallas_call(
        hand_over,
        name="hand_over",
        out_shape=(
            shape((ticks, *block), BF16),
            shape((ticks, *block), BF16),
            shape((SIDE, chunk, cols), BF16),
            shape((SIDE, chunk, cols), BF16),
        ),
        in_specs=[any_space] * 4,
        out_specs=(any_space,) * 4,
        scratch_shapes=[
            vmem((ticks, *block), BF16),
            vmem((ticks, *block), BF16),
            vmem((SIDE, chunk, cols), BF16),
            vmem((SIDE, chunk, cols), BF16),
            dma((2, 4)),
        ],
    )(f_out, b_out, w_out, m_out)
    return (
        f_out[None, None],
        b_out[None, None],
        w_out.reshape(1, part_rows, cols),
        m_out.reshape(1, part_rows, cols),
    )


def solution(mesh):
    return jax.shard_map(
        body,
        mesh=mesh,
        in_specs=(
            P("section", None, "tensor"),
            P("section", "dp", "tensor"),
            P("section", "dp", "tensor"),
            P("dp", "section", None, "tensor"),
            P("dp", None, None, "tensor"),
            P("dp", "section", None, "tensor"),
            P("dp", None, None, "tensor"),
            P("dp", "section", None, None, "tensor"),
        ),
        out_specs=(
            P("dp", "section", None, None, "tensor"),
            P("dp", "section", None, None, "tensor"),
            P("section", "dp", "tensor"),
            P("section", "dp", "tensor"),
        ),
        check_vma=False,
    )
```
